8 devices in a mesh: dp: 1 (over z), tp: 8 (over y, x, core).
Axes of the slice: x: 2, y: 2, z: 1, core: 2. Of those that a mesh axis runs over, the one named last changes fastest.
Arguments:
- hidden: bfloat16 [16, 64, 2048], P('dp')
- tree_mask: int32 [16, 64, 64], P('dp')
- depth: int32 [16, 64], P('dp')
- ctx_len: int32 [16], P('dp')
- block_table: int32 [16, 12], P('dp')
- score_id: int32 [16, 64], P('dp')
- k_cache: bfloat16 [192, 16, 8, 64], P('dp', None, 'tp')
- v_cache: bfloat16 [192, 16, 8, 64], P('dp', None, 'tp')
- attn_norm: bfloat16 [2048], replicated
- w_q: bfloat16 [2048, 2048], P(None, 'tp')
- w_k: bfloat16 [2048, 512], P(None, 'tp')
- w_v: bfloat16 [2048, 512], P(None, 'tp')
- w_o: bfloat16 [2048, 2048], P('tp')
- mlp_norm: bfloat16 [2048], replicated
- w_gate: bfloat16 [2048, 8192], P(None, 'tp')
- w_up: bfloat16 [2048, 8192], P(None, 'tp')
- w_down: bfloat16 [8192, 2048], P('tp')
- final_norm: bfloat16 [2048], replicated
- w_lm: bfloat16 [2048, 128256], P(None, 'tp')
Outputs:
- output 1: float32 [16, 64], P('dp')
- output 2: float32 [16, 64], P('dp')
- output 3: bfloat16 [192, 16, 8, 64], P('dp', None, 'tp')
- output 4: bfloat16 [192, 16, 8, 64], P('dp', None, 'tp')
All inputs are finite; a program needn't handle non-finite values.
Results may differ from the reference program's by a relative error of at most 0.00334518.
Values are sent between devices in bfloat16 or wider.
A program may use at most 1 GiB of HBM per device.

```python
import math
import jax
import jax.numpy as jnp
from jax import lax

REQUESTS = 16
NODES = 64
PAGES = 12
PAGE_SIZE = 16
MODEL_DIM = 2048
HEADS = 32
KV_HEADS = 8
HEAD_DIM = 64
FFN_DIM = 8192
VOCAB_SIZE = 128256
ROPE_THETA = 500000
RMS_EPS = 1e-5
BLOCKS = REQUESTS * PAGES
SPAN = PAGES * PAGE_SIZE
MAX_CTX = SPAN - NODES
GROUP = HEADS // KV_HEADS


def draw_routing(key):
    k_spread, k_step, k_ctx, k_table, k_score = jax.random.split(key, 5)
    spread = jax.random.randint(k_spread, (REQUESTS, 1), 1, 4)
    step = jnp.minimum(jax.random.randint(k_step, (REQUESTS, NODES), 0, 4), spread)
    node_ids = jnp.arange(NODES)
    parent = jnp.maximum(node_ids[None, :] - 1 - step, 0)
    linked = (parent[:, :, None] == node_ids[None, None, :]) & (node_ids[None, :, None] > 0)
    reach = linked | (node_ids[:, None] == node_ids[None, :])[None]
    for _ in range(int(math.log2(NODES)) + 1):
        reach = jnp.any(reach[:, :, :, None] & reach[:, None, :, :], axis=2)
    tree_mask = reach.astype(jnp.int32)
    depth = jnp.sum(tree_mask, axis=-1).astype(jnp.int32) - 1
    ctx_len = jax.random.randint(k_ctx, (REQUESTS,), 1, MAX_CTX + 1).astype(jnp.int32)
    ctx_len = ctx_len.at[0].set(MAX_CTX)
    block_table = jax.random.permutation(k_table, BLOCKS).astype(jnp.int32).reshape(REQUESTS, PAGES)
    score_id = jax.random.randint(k_score, (REQUESTS, NODES), 0, VOCAB_SIZE).astype(jnp.int32)
    score_id = score_id.at[0, 0].set(VOCAB_SIZE - 1)
    return tree_mask, depth, ctx_len, block_table, score_id


def normal_weight(key, shape, scale):
    return (scale * jax.random.normal(key, shape, jnp.float32)).astype(jnp.bfloat16)


def gain_vector(key):
    return (1.0 + 0.3 * jax.random.normal(key, (MODEL_DIM,), jnp.float32)).astype(jnp.bfloat16)


def setup_inputs(seed: int = 0, part: int = 0) -> dict:
    part_key = jax.random.fold_in(jax.random.key(seed), part)
    keys = jax.random.split(part_key, 4)
    tree_mask, depth, ctx_len, block_table, score_id = draw_routing(keys[0])
    shared = jax.random.split(jax.random.key(seed + 1), 11)
    cache_shape = (BLOCKS, PAGE_SIZE, KV_HEADS, HEAD_DIM)
    return {
        "hidden": normal_weight(keys[1], (REQUESTS, NODES, MODEL_DIM), 1.0),
        "tree_mask": tree_mask,
        "depth": depth,
        "ctx_len": ctx_len,
        "block_table": block_table,
        "score_id": score_id,
        "k_cache": normal_weight(keys[2], cache_shape, 1.0),
        "v_cache": normal_weight(keys[3], cache_shape, 1.0),
        "attn_norm": gain_vector(shared[0]),
        "w_q": normal_weight(shared[1], (MODEL_DIM, HEADS * HEAD_DIM), 2.5 * MODEL_DIM ** -0.5),
        "w_k": normal_weight(shared[2], (MODEL_DIM, KV_HEADS * HEAD_DIM), 1.5 * MODEL_DIM ** -0.5),
        "w_v": normal_weight(shared[3], (MODEL_DIM, KV_HEADS * HEAD_DIM), MODEL_DIM ** -0.5),
        "w_o": normal_weight(shared[4], (HEADS * HEAD_DIM, MODEL_DIM), 1.5 * (HEADS * HEAD_DIM) ** -0.5),
        "mlp_norm": gain_vector(shared[5]),
        "w_gate": normal_weight(shared[6], (MODEL_DIM, FFN_DIM), MODEL_DIM ** -0.5),
        "w_up": normal_weight(shared[7], (MODEL_DIM, FFN_DIM), MODEL_DIM ** -0.5),
        "w_down": normal_weight(shared[8], (FFN_DIM, MODEL_DIM), 1.5 * FFN_DIM ** -0.5),
        "final_norm": gain_vector(shared[9]),
        "w_lm": normal_weight(shared[10], (MODEL_DIM, VOCAB_SIZE), 3.0 * MODEL_DIM ** -0.5),
    }


def rms_norm(values, gain):
    widened = values.astype(jnp.float32)
    scale = lax.rsqrt(jnp.mean(widened * widened, axis=-1, keepdims=True) + RMS_EPS)
    return (widened * scale * gain.astype(jnp.float32)).astype(jnp.bfloat16)


def rotate(values, positions):
    head_dim = values.shape[-1]
    half = head_dim // 2
    inv_freq = 1.0 / (ROPE_THETA ** (jnp.arange(half, dtype=jnp.float32) * (2.0 / head_dim)))
    angles = positions.astype(jnp.float32)[..., None] * inv_freq
    cosine = jnp.cos(angles)[..., None, :]
    sine = jnp.sin(angles)[..., None, :]
    first = values[..., :half]
    second = values[..., half:]
    return jnp.concatenate([first * cosine - second * sine, second * cosine + first * sine], axis=-1)


def reference(hidden, tree_mask, depth, ctx_len, block_table, score_id, k_cache, v_cache, attn_norm, w_q, w_k, w_v, w_o, mlp_norm, w_gate, w_up, w_down, final_norm, w_lm):
    scale = HEAD_DIM ** -0.5
    slot_ids = jnp.arange(SPAN)

    def one_request(item):
        rows, mask_row, depth_row, context, table_row, targets = item
        normed = rms_norm(rows, attn_norm)
        positions = context + depth_row
        query = jnp.dot(normed, w_q, preferred_element_type=jnp.float32).reshape(NODES, HEADS, HEAD_DIM)
        query = rotate(query, positions).astype(jnp.bfloat16).reshape(NODES, KV_HEADS, GROUP, HEAD_DIM)
        key_new = jnp.dot(normed, w_k, preferred_element_type=jnp.float32).reshape(NODES, KV_HEADS, HEAD_DIM)
        key_new = rotate(key_new, positions).astype(jnp.bfloat16)
        val_new = jnp.dot(normed, w_v, preferred_element_type=jnp.float32).astype(jnp.bfloat16).reshape(NODES, KV_HEADS, HEAD_DIM)
        key_old = k_cache[table_row].reshape(SPAN, KV_HEADS, HEAD_DIM)
        val_old = v_cache[table_row].reshape(SPAN, KV_HEADS, HEAD_DIM)
        query_wide = query.astype(jnp.float32)
        score_old = jnp.einsum("tkgh,skh->tkgs", query_wide, key_old.astype(jnp.float32)) * scale
        score_old = jnp.where((slot_ids < context)[None, None, None, :], score_old, -jnp.inf)
        score_new = jnp.einsum("tkgh,jkh->tkgj", query_wide, key_new.astype(jnp.float32)) * scale
        score_new = jnp.where((mask_row > 0)[:, None, None, :], score_new, -jnp.inf)
        top = jnp.maximum(jnp.max(score_old, axis=-1), jnp.max(score_new, axis=-1))[..., None]
        prob_old = jnp.exp(score_old - top)
        prob_new = jnp.exp(score_new - top)
        total = jnp.sum(prob_old, axis=-1) + jnp.sum(prob_new, axis=-1)
        mixed = jnp.einsum("tkgs,skh->tkgh", prob_old.astype(jnp.bfloat16).astype(jnp.float32), val_old.astype(jnp.float32))
        mixed = mixed + jnp.einsum("tkgj,jkh->tkgh", prob_new.astype(jnp.bfloat16).astype(jnp.float32), val_new.astype(jnp.float32))
        attended = (mixed / total[..., None]).astype(jnp.bfloat16).reshape(NODES, HEADS * HEAD_DIM)
        attn_out = jnp.dot(attended, w_o, preferred_element_type=jnp.float32).astype(jnp.bfloat16)
        residual = (rows.astype(jnp.float32) + attn_out.astype(jnp.float32)).astype(jnp.bfloat16)
        normed_mlp = rms_norm(residual, mlp_norm)
        gate = jnp.dot(normed_mlp, w_gate, preferred_element_type=jnp.float32)
        upper = jnp.dot(normed_mlp, w_up, preferred_element_type=jnp.float32)
        product = (jax.nn.silu(gate) * upper).astype(jnp.bfloat16)
        mlp_out = jnp.dot(product, w_down, preferred_element_type=jnp.float32).astype(jnp.bfloat16)
        layer_out = (residual.astype(jnp.float32) + mlp_out.astype(jnp.float32)).astype(jnp.bfloat16)
        logits = jnp.dot(rms_norm(layer_out, final_norm), w_lm, preferred_element_type=jnp.float32)
        log_norm = jax.nn.logsumexp(logits, axis=-1)
        picked = jnp.take_along_axis(logits, targets[:, None], axis=-1)[:, 0]
        return log_norm, picked - log_norm, key_new, val_new

    log_norm, log_prob, key_new, val_new = lax.map(one_request, (hidden, tree_mask, depth, ctx_len, block_table, score_id))
    slots = ctx_len[:, None] + jnp.arange(NODES)[None, :]
    slot_blocks = jnp.take_along_axis(block_table, slots // PAGE_SIZE, axis=1)
    k_out = k_cache.at[slot_blocks, slots % PAGE_SIZE].set(key_new)
    v_out = v_cache.at[slot_blocks, slots % PAGE_SIZE].set(val_new)
    return (log_norm, log_prob, k_out, v_out)
```

```python
import functools

import jax
import jax.numpy as jnp
import numpy as np
from jax import lax
from jax.experimental import pallas as pl
from jax.experimental.pallas import tpu as pltpu
from jax.sharding import PartitionSpec as P

RMS_EPS = 1e-5
ROPE_THETA = 500000
DIM = 2048
ROWS = 1024
NODES = 64
PAGES = 12
PAGE = 16
SPAN = PAGES * PAGE
HD = 64
FFN = 1024
VOCAB = 16032
TILE = 1024
FULL_TILES = 15
LAST = 640
TAIL_AT = 16000
CHUNKS = 2
CR = ROWS // CHUNKS
HALF = CR // 2
BR = CR // 8
MESH = pl.DeviceIdType.MESH
F32 = jnp.float32
BF16 = jnp.bfloat16


def rope_table():
    half = HD // 2
    freq = (np.float32(1.0) / np.power(np.float32(ROPE_THETA), np.arange(half, dtype=np.float32) * np.float32(2.0 / HD))).astype(np.float32)
    angle = (np.arange(SPAN, dtype=np.float32)[:, None] * freq[None, :]).astype(np.float32).astype(np.float64)
    cos = np.tile(np.cos(angle), (1, 4)).astype(np.float32)
    sin = np.sin(angle)
    sin = np.concatenate([-sin, sin, -sin, sin], axis=1).astype(np.float32)
    table = np.concatenate([cos, sin], axis=1)
    high = table.astype(jnp.bfloat16)
    rest = table - high.astype(np.float32)
    mid = rest.astype(jnp.bfloat16)
    low = (rest - mid.astype(np.float32)).astype(jnp.bfloat16)
    return np.concatenate([high, mid, low], axis=1)


def normalize(values, gain):
    scale = lax.rsqrt(jnp.mean(values * values, axis=-1, keepdims=True) + RMS_EPS)
    return (values * scale * gain).astype(BF16)


def dot(a, b):
    return jnp.dot(a, b, preferred_element_type=F32)


def dot_nt(a, b):
    return lax.dot_general(a, b, (((1,), (1,)), ((), ())), preferred_element_type=F32)


def dot_tn(a, b):
    return lax.dot_general(a, b, (((0,), (0,)), ((), ())), preferred_element_type=F32)


def attention_kernel(group, ctx_ref, bt_ref, hid_ref, depth_ref, mask_ref, gain_ref, wq_ref, wkv_ref, table_ref, kv_ref, att_ref, kvout_ref, old_ref):
    step = pl.program_id(0)
    normed = normalize(hid_ref[...].astype(F32), gain_ref[...].astype(F32))
    q_all = dot(normed, wq_ref[...])
    kv_all = dot(normed, wkv_ref[...])
    lane = lax.broadcasted_iota(jnp.int32, (1, 128), 1)
    low = lane < 64
    first = (lane % 64) < 32

    def rope(values, cosine, sine):
        swapped = jnp.where(first, pltpu.roll(values, 96, 1), pltpu.roll(values, 32, 1))
        return values * cosine + swapped * sine

    for i in range(group):
        b = step * group + i
        ctx = ctx_ref[b]
        rows = slice(i * NODES, (i + 1) * NODES)
        position = depth_ref[i] + ctx
        hot = (lax.broadcasted_iota(jnp.int32, (SPAN, NODES), 0) == position).astype(F32).astype(BF16)
        looked = dot_tn(hot, table_ref[...])
        both = looked[:, :256] + looked[:, 256:512] + looked[:, 512:]
        cosine, sine = both[:, :128], both[:, 128:]
        q01 = (rope(q_all[rows, :128], cosine, sine) * 0.125).astype(BF16)
        q23 = (rope(q_all[rows, 128:], cosine, sine) * 0.125).astype(BF16)
        kv_new = rope(kv_all[rows], jnp.where(low, cosine, 1.0), jnp.where(low, sine, 0.0)).astype(BF16)
        for p in range(PAGES):
            old_ref[i, p * PAGE:(p + 1) * PAGE, :] = kv_ref[bt_ref[b, p]].astype(F32)
        slot = lax.broadcasted_iota(jnp.int32, (SPAN, NODES), 0)
        node = lax.broadcasted_iota(jnp.int32, (SPAN, NODES), 1)
        place = (slot - node == ctx).astype(F32).astype(BF16)
        shifted = dot(place, kv_new)
        slot_col = lax.broadcasted_iota(jnp.int32, (SPAN, 128), 0)
        fresh = (slot_col >= ctx) & (slot_col < ctx + NODES)
        merged = jnp.where(fresh, shifted, old_ref[i])
        merged16 = merged.astype(BF16)
        for p in range(PAGES):
            kvout_ref[bt_ref[b, p]] = merged16[p * PAGE:(p + 1) * PAGE]
        turned = pltpu.roll(merged, 64, 1)
        k_even = jnp.where(low, merged, 0.0).astype(BF16)
        v_odd = jnp.where(low, 0.0, merged).astype(BF16)
        v_even = jnp.where(low, turned, 0.0).astype(BF16)
        k_odd = jnp.where(low, 0.0, turned).astype(BF16)
        tree = dot_nt(mask_ref[i].astype(F32).astype(BF16), place)
        slot_row = lax.broadcasted_iota(jnp.int32, (NODES, SPAN), 1)
        seen = (slot_row < ctx) | (tree > 0.5)

        def head(query, keys):
            score = jnp.where(seen, dot_nt(query, keys), -jnp.inf)
            weight = jnp.exp(score - jnp.max(score, axis=-1, keepdims=True))
            return weight.astype(BF16), jnp.sum(weight, axis=-1, keepdims=True)

        for pair, query in enumerate((q01, q23)):
            w_even, t_even = head(query, k_even)
            w_odd, t_odd = head(query, k_odd)
            mixed = dot(w_even, v_even) + dot(w_odd, v_odd)
            att_ref[rows, pair * 128:(pair + 1) * 128] = (mixed / jnp.where(low, t_even, t_odd)).astype(BF16)


def attention(hidden, tree_mask, depth, ctx_len, block_table, kv_cache, attn_norm, w_q, w_kv, table):
    group = 4
    grid = (hidden.shape[0] // (group * NODES),)
    spec = pltpu.PrefetchScalarGridSpec(
        num_scalar_prefetch=2,
        grid=grid,
        in_specs=[
            pl.BlockSpec((group * NODES, DIM), lambda i, *_: (i, 0)),
            pl.BlockSpec((group, 1, NODES), lambda i, *_: (i, 0, 0)),
            pl.BlockSpec((group, NODES, NODES), lambda i, *_: (i, 0, 0)),
            pl.BlockSpec((1, DIM), lambda i, *_: (0, 0)),
            pl.BlockSpec((DIM, 256), lambda i, *_: (0, 0)),
            pl.BlockSpec((DIM, 128), lambda i, *_: (0, 0)),
            pl.BlockSpec(table.shape, lambda i, *_: (0, 0)),
            pl.BlockSpec(kv_cache.shape, lambda i, *_: (0, 0, 0)),
        ],
        out_specs=[
            pl.BlockSpec((group * NODES, 256), lambda i, *_: (i, 0)),
            pl.BlockSpec(kv_cache.shape, lambda i, *_: (0, 0, 0)),
        ],
        scratch_shapes=[pltpu.VMEM((group, SPAN, 128), F32)],
    )
    return pl.pallas_call(
        functools.partial(attention_kernel, group),
        grid_spec=spec,
        out_shape=[jax.ShapeDtypeStruct((hidden.shape[0], 256), BF16), jax.ShapeDtypeStruct(kv_cache.shape, BF16)],
        compiler_params=pltpu.CompilerParams(vmem_limit_bytes=40 * 2**20),
        name="attention",
    )(ctx_len, block_table, hidden, depth, tree_mask, attn_norm, w_q, w_kv, table, kv_cache)


def layer_kernel(att, wo, hid, mgain, wg_hbm, wu_hbm, wd_hbm, fgain, wlm, wtail, sid, ln_ref, lp_ref,
                 wg, wu, wd, wbuf, psib, pown, s1buf, s2buf, mfull, hown, pact, mrun, srun, prun, stat,
                 load_sem, tile_sem, s1_send, s1_recv, s2_send, s2_recv, ag_send, ag_recv, fw_send, fw_recv, fin_send, fin_recv):
    me = lax.axis_index("tp")
    core = me % 2
    chip = me // 2
    cx = chip % 2
    cy = chip // 2
    sib = me + 1 - 2 * core
    far = (chip + 1 - 2 * cx, chip + 2 - 4 * cy, 3 - chip)

    def peer(rel):
        return 2 * far[rel] + core

    def remote(src, dst, ssem, rsem, target):
        return pltpu.make_async_remote_copy(src_ref=src, dst_ref=dst, send_sem=ssem, recv_sem=rsem, device_id={"tp": target}, device_id_type=MESH)

    barrier = pltpu.get_barrier_semaphore()
    for off in range(1, 8):
        pl.semaphore_signal(barrier, inc=1, device_id={"tp": (me + off) % 8}, device_id_type=MESH)

    loads = [
        pltpu.make_async_copy(wg_hbm, wg, load_sem.at[0]),
        pltpu.make_async_copy(wu_hbm, wu, load_sem.at[1]),
        pltpu.make_async_copy(wd_hbm, wd, load_sem.at[2]),
    ]

    def own_rows(c):
        return c * CR + (core * 4 + chip) * BR

    hid_loads = [
        pltpu.make_async_copy(hid.at[pl.ds(pl.multiple_of(own_rows(c), BR), BR)], hown.at[pl.ds(c * BR, BR)], load_sem.at[3 + c])
        for c in range(CHUNKS)
    ]
    for copy in hid_loads + loads:
        copy.start()

    def tile_copy(t, j):
        return pltpu.make_async_copy(wlm.at[:, pl.ds(pl.multiple_of(j * TILE, TILE), TILE)], wbuf.at[t % 3], tile_sem.at[t % 3])

    def last_copy(t):
        return pltpu.make_async_copy(wlm.at[:, pl.ds(FULL_TILES * TILE, LAST)], wbuf.at[t % 3, :, pl.ds(0, LAST)], tile_sem.at[t % 3])

    tile_copy(0, 0).start()
    tile_copy(1, 1).start()

    mrun[...] = jnp.full_like(mrun, -jnp.inf)
    srun[...] = jnp.zeros_like(srun)
    prun[...] = jnp.zeros_like(prun)

    def half_rows(c, which):
        return pl.ds(pl.multiple_of(c * CR + which * HALF, HALF), HALF)

    def slab(c):
        return pl.ds(c * HALF, HALF)

    def first_copy(s, c):
        return remote(psib.at[s, slab(c)], s1buf.at[s, slab(c)], s1_send.at[s, c], s1_recv.at[s, c], sib)

    def project(c):
        psib[0, slab(c)] = dot(att[half_rows(c, 1 - core)], wo[...]).astype(BF16)
        if c == 0:
            pl.semaphore_wait(barrier, 7)
        first_copy(0, c).start()
        pown[0, slab(c)] = dot(att[half_rows(c, core)], wo[...]).astype(BF16)

    def second_copy(s, c, rel):
        block = pl.ds(pl.multiple_of(c * HALF + far[rel] * BR, BR), BR)
        return remote(pown.at[s, block], s2buf.at[s, c, rel], s2_send.at[s, c, rel], s2_recv.at[s, c, rel], peer(rel))

    def pair_sum(s, c):
        first_copy(s, c).wait_recv()
        pown[s, slab(c)] = (pown[s, slab(c)].astype(F32) + s1buf[s, slab(c)].astype(F32)).astype(BF16)
        for rel in range(3):
            second_copy(s, c, rel).start()

    def block_rows(c, k, q):
        return pl.ds(pl.multiple_of(c * CR + (k * 4 + q) * BR, BR), BR)

    def gather_copy(s, c, rel, rows):
        target = sib if rel == 3 else peer(rel)
        return remote(mfull.at[s, rows], mfull.at[s, rows], ag_send.at[s, c, rel], ag_recv.at[s, c, rel], target)

    def forward_copy(s, c, rel, rows):
        return remote(mfull.at[s, rows], mfull.at[s, rows], fw_send.at[s, c, rel], fw_recv.at[s, c, rel], sib)

    def finish_sum(s, c):
        for rel in range(3):
            second_copy(s, c, rel).wait_recv()
        total = pown[s, pl.ds(pl.multiple_of(c * HALF + chip * BR, BR), BR)].astype(F32)
        for rel in range(3):
            total = total + s2buf[s, c, rel].astype(F32)
        if s == 0:
            hid_loads[c].wait()
        rows = pl.ds(c * BR, BR)
        state = (hown[rows].astype(F32) + total.astype(BF16).astype(F32)).astype(BF16)
        if s == 0:
            hown[rows] = state
        gain = (mgain if s == 0 else fgain)[...].astype(F32)
        mine = block_rows(c, core, chip)
        mfull[s, mine] = normalize(state.astype(F32), gain)
        for rel in range(4):
            gather_copy(s, c, rel, mine).start()

    def forward(s, c):
        for rel in range(3):
            rows = block_rows(c, core, far[rel])
            gather_copy(s, c, rel, rows).wait_recv()
            forward_copy(s, c, rel, rows).start()

    def complete(s, c):
        gather_copy(s, c, 3, block_rows(c, 1 - core, chip)).wait_recv()
        for rel in range(3):
            forward_copy(s, c, rel, block_rows(c, 1 - core, far[rel])).wait_recv()

    def mlp(c):
        if c == 0:
            for copy in loads:
                copy.wait()

        def up(j, carry):
            cols = pl.ds(pl.multiple_of(j * 256, 256), 256)
            values = mfull[0, pl.ds(c * CR, CR)]
            gate = dot(values, wg[:, cols])
            upper = dot(values, wu[:, cols])
            pact[:, cols] = (gate * (1.0 / (1.0 + jnp.exp(-gate))) * upper).astype(BF16)
            return carry

        lax.fori_loop(0, FFN // 256, up, 0)

        def down(which, out):
            rows = pl.ds(pl.multiple_of(which * HALF, HALF), HALF)

            def one(j, carry):
                cols = pl.ds(pl.multiple_of(j * 512, 512), 512)
                out[1, slab(c), cols] = dot(pact[rows], wd[:, cols]).astype(BF16)
                return carry

            lax.fori_loop(0, DIM // 512, one, 0)

        down(1 - core, psib)
        first_copy(1, c).start()
        down(core, pown)

    lane = lax.broadcasted_iota(jnp.int32, (1, 128), 1)

    def absorb(rows, values, weights, col0, valid_last):
        logits = dot(values, weights)
        groups = [logits[:, g * 128:(g + 1) * 128] for g in range(weights.shape[1] // 128)]
        if valid_last is not None:
            groups[-1] = jnp.where(lane < valid_last, groups[-1], -jnp.inf)
        wanted = sid[rows] - (me * VOCAB + col0)
        before = mrun[rows]
        top = before
        for x in groups:
            top = jnp.maximum(top, x)
        total = srun[rows] * jnp.exp(before - top)
        picked = prun[rows]
        for g, x in enumerate(groups):
            total = total + jnp.exp(x - top)
            hit = lane == wanted - g * 128
            if valid_last is not None and g == len(groups) - 1:
                hit = hit & (lane < valid_last)
            picked = picked + jnp.where(hit, x, 0.0)
        mrun[rows] = top
        srun[rows] = total
        prun[rows] = picked

    def vocab(c, events):
        rows = pl.ds(c * CR, CR)

        def step(j, carry):
            t = c * (FULL_TILES + 1) + j

            @pl.when(j + 2 < FULL_TILES)
            def _():
                tile_copy(t + 2, j + 2).start()

            @pl.when(j + 2 == FULL_TILES)
            def _():
                last_copy(t + 2).start()

            if c + 1 < CHUNKS:
                @pl.when(j + 2 > FULL_TILES)
                def _():
                    tile_copy(t + 2, 0).start()

            tile_copy(t, j).wait()
            slot = t % 3
            for n in range(TILE // 256):
                absorb(rows, mfull[1, rows], wbuf[slot, :, n * 256:(n + 1) * 256], j * TILE + n * 256, None)
            return carry

        at = 0
        for stop in sorted(events) + [FULL_TILES]:
            if stop > at:
                lax.fori_loop(at, stop, step, 0)
            at = stop
            for event in events.get(stop, ()):
                event()
        t = c * (FULL_TILES + 1) + FULL_TILES
        if c + 1 < CHUNKS:
            tile_copy(t + 2, 1).start()
        last_copy(t).wait()
        slot = t % 3
        base = FULL_TILES * TILE
        absorb(rows, mfull[1, rows], wbuf[slot, :, 0:256], base, None)
        absorb(rows, mfull[1, rows], wbuf[slot, :, 256:512], base + 256, None)
        tail = jnp.concatenate([wbuf[slot, :, 512:640], wtail[...]], axis=1)
        absorb(rows, mfull[1, rows], tail, base + 512, VOCAB - TAIL_AT)

    project(0)
    project(1)
    pair_sum(0, 0)
    finish_sum(0, 0)
    pair_sum(0, 1)
    forward(0, 0)
    complete(0, 0)
    mlp(0)
    pair_sum(1, 0)
    finish_sum(0, 1)
    finish_sum(1, 0)
    forward(0, 1)
    complete(0, 1)
    mlp(1)
    forward(1, 0)
    complete(1, 0)
    vocab(0, {
        1: (lambda: pair_sum(1, 1),),
        7: (lambda: finish_sum(1, 1),),
        13: (lambda: forward(1, 1),),
    })
    complete(1, 1)
    vocab(1, {})

    for i in range(8):
        rows = pl.ds(i * 128, 128)
        tops = mrun[rows]
        top = jnp.max(tops.T, axis=0, keepdims=True)
        column = jnp.max(tops, axis=1, keepdims=True)
        sums = srun[rows] * jnp.exp(tops - column)
        stat[0, pl.ds(i, 1)] = top
        stat[0, pl.ds(8 + i, 1)] = jnp.sum(sums.T, axis=0, keepdims=True)
        stat[0, pl.ds(16 + i, 1)] = jnp.sum(prun[rows].T, axis=0, keepdims=True)

    def stat_copy(off):
        return remote(stat.at[0], stat.at[off], fin_send.at[off - 1], fin_recv.at[off - 1], (me + off) % 8)

    for off in range(1, 8):
        stat_copy(off).start()
    for off in range(1, 8):
        stat_copy(off).wait_recv()
    top = stat[0, 0:8]
    for off in range(1, 8):
        top = jnp.maximum(top, stat[off, 0:8])
    total = jnp.zeros_like(top)
    picked = jnp.zeros_like(top)
    for off in range(8):
        total = total + stat[off, 8:16] * jnp.exp(stat[off, 0:8] - top)
        picked = picked + stat[off, 16:24]
    log_norm = top + jnp.log(total)
    log_prob = picked - log_norm
    for ref, values in ((ln_ref, log_norm), (lp_ref, log_prob)):
        for i in range(8):
            ref[pl.ds(2 * i, 1), :] = values[i:i + 1, 0:64]
            ref[pl.ds(2 * i + 1, 1), :] = values[i:i + 1, 64:128]

    for s in range(2):
        for c in range(CHUNKS):
            first_copy(s, c).wait_send()
            mine = block_rows(c, core, chip)
            for rel in range(4):
                gather_copy(s, c, rel, mine).wait_send()
            for rel in range(3):
                second_copy(s, c, rel).wait_send()
                forward_copy(s, c, rel, block_rows(c, core, far[rel])).wait_send()
    for off in range(1, 8):
        stat_copy(off).wait_send()


def layer(att, w_o, hidden, mlp_norm, w_gate, w_up, w_down, final_norm, w_lm, w_tail, score_id):
    vmem = pl.BlockSpec(memory_space=pltpu.VMEM)
    hbm = pl.BlockSpec(memory_space=pl.ANY)
    sem = pltpu.SemaphoreType.DMA
    return pl.pallas_call(
        layer_kernel,
        in_specs=[vmem, vmem, hbm, vmem, hbm, hbm, hbm, vmem, hbm, vmem, vmem],
        out_specs=[vmem, vmem],
        out_shape=[jax.ShapeDtypeStruct((16, NODES), F32)] * 2,
        scratch_shapes=[
            pltpu.VMEM((DIM, FFN), BF16),
            pltpu.VMEM((DIM, FFN), BF16),
            pltpu.VMEM((FFN, DIM), BF16),
            pltpu.VMEM((3, DIM, TILE), BF16),
            pltpu.VMEM((2, ROWS // 2, DIM), BF16),
            pltpu.VMEM((2, ROWS // 2, DIM), BF16),
            pltpu.VMEM((2, ROWS // 2, DIM), BF16),
            pltpu.VMEM((2, CHUNKS, 3, BR, DIM), BF16),
            pltpu.VMEM((2, ROWS, DIM), BF16),
            pltpu.VMEM((ROWS // 8, DIM), BF16),
            pltpu.VMEM((CR, FFN), BF16),
            pltpu.VMEM((ROWS, 128), F32),
            pltpu.VMEM((ROWS, 128), F32),
            pltpu.VMEM((ROWS, 128), F32),
            pltpu.VMEM((8, 24, 128), F32),
            sem((3 + CHUNKS,)),
            sem((3,)),
            sem((2, CHUNKS)),
            sem((2, CHUNKS)),
            sem((2, CHUNKS, 3)),
            sem((2, CHUNKS, 3)),
            sem((2, CHUNKS, 4)),
            sem((2, CHUNKS, 4)),
            sem((2, CHUNKS, 3)),
            sem((2, CHUNKS, 3)),
            sem((7,)),
            sem((7,)),
        ],
        compiler_params=pltpu.CompilerParams(collective_id=0, has_side_effects=True, vmem_limit_bytes=63 * 2**20),
        name="layer",
    )(att, w_o, hidden, mlp_norm, w_gate, w_up, w_down, final_norm, w_lm, w_tail, score_id)


def solution(mesh):
    def group_step(hidden, tree_mask, depth, ctx_len, block_table, score_id, k_cache, v_cache, attn_norm, w_q, w_k, w_v, w_o, mlp_norm, w_gate, w_up, w_down, final_norm, w_lm):
        flat = hidden.reshape(ROWS, DIM)
        kv_cache = jnp.concatenate([k_cache[:, :, 0], v_cache[:, :, 0]], axis=-1)
        w_kv = jnp.concatenate([w_k, w_v], axis=1)
        table = jnp.asarray(rope_table())
        att, kv_out = attention(flat, tree_mask, depth[:, None, :], ctx_len, block_table, kv_cache, attn_norm[None], w_q, w_kv, table)
        w_tail = jnp.pad(w_lm[:, TAIL_AT:], ((0, 0), (0, 128 - (VOCAB - TAIL_AT))))
        log_norm, log_prob = layer(att, w_o, flat, mlp_norm[None], w_gate, w_up, w_down, final_norm[None], w_lm, w_tail, score_id.reshape(ROWS, 1))
        return log_norm, log_prob, kv_out[:, :, None, :HD], kv_out[:, :, None, HD:]

    request_spec = P("dp", None, None)
    node_spec = P("dp", None)
    cache_spec = P("dp", None, "tp", None)
    shared_spec = P(None)
    column_spec = P(None, "tp")
    row_spec = P("tp", None)
    in_specs = (request_spec, request_spec, node_spec, P("dp"), node_spec, node_spec, cache_spec, cache_spec, shared_spec, column_spec, column_spec, column_spec, row_spec, shared_spec, column_spec, column_spec, row_spec, shared_spec, column_spec)
    out_specs = (node_spec, node_spec, cache_spec, cache_spec)
    return jax.shard_map(group_step, mesh=mesh, in_specs=in_specs, out_specs=out_specs, check_vma=False)
```

```python
import functools

import jax
import jax.numpy as jnp
import numpy as np
from jax import lax
from jax.experimental import pallas as pl
from jax.experimental.pallas import tpu as pltpu
from jax.sharding import PartitionSpec as P

RMS_EPS = 1e-5
ROPE_THETA = 500000
DIM = 2048
ROWS = 1024
NODES = 64
PAGES = 12
PAGE = 16
SPAN = PAGES * PAGE
HD = 64
FFN = 1024
VOCAB = 16032
TILE = 1008
TILES = 16
REPEAT = TILES * TILE - VOCAB
LOWEST = -3e38
CHUNKS = 2
CR = ROWS // CHUNKS
HALF = CR // 2
BR = CR // 8
MESH = pl.DeviceIdType.MESH
F32 = jnp.float32
BF16 = jnp.bfloat16


def rope_table():
    half = HD // 2
    freq = (np.float32(1.0) / np.power(np.float32(ROPE_THETA), np.arange(half, dtype=np.float32) * np.float32(2.0 / HD))).astype(np.float32)
    angle = (np.arange(SPAN, dtype=np.float32)[:, None] * freq[None, :]).astype(np.float32).astype(np.float64)
    cos = np.tile(np.cos(angle), (1, 4)).astype(np.float32)
    sin = np.sin(angle)
    sin = np.concatenate([-sin, sin, -sin, sin], axis=1).astype(np.float32)
    table = np.concatenate([cos, sin], axis=1)
    high = table.astype(jnp.bfloat16)
    rest = table - high.astype(np.float32)
    mid = rest.astype(jnp.bfloat16)
    low = (rest - mid.astype(np.float32)).astype(jnp.bfloat16)
    return np.concatenate([high, mid, low], axis=1)


def normalize(values, gain):
    scale = lax.rsqrt(jnp.mean(values * values, axis=-1, keepdims=True) + RMS_EPS)
    return (values * scale * gain).astype(BF16)


def dot(a, b):
    return jnp.dot(a, b, preferred_element_type=F32)


def dot_nt(a, b):
    return lax.dot_general(a, b, (((1,), (1,)), ((), ())), preferred_element_type=F32)


def dot_tn(a, b):
    return lax.dot_general(a, b, (((0,), (0,)), ((), ())), preferred_element_type=F32)


def attention_kernel(group, ctx_ref, bt_ref, hid_ref, depth_ref, mask_ref, gain_ref, wq_ref, wk_ref, wv_ref, table_ref, kv_ref, att_ref, kvout_ref, old_ref):
    step = pl.program_id(0)
    normed = normalize(hid_ref[...].astype(F32), gain_ref[...].astype(F32))
    q_all = dot(normed, wq_ref[...])
    kv_all = dot_nt(normed, jnp.concatenate([wk_ref[...], wv_ref[...]], axis=0))
    lane = lax.broadcasted_iota(jnp.int32, (1, 128), 1)
    low = lane < 64
    first = (lane % 64) < 32

    def rope(values, cosine, sine):
        swapped = jnp.where(first, pltpu.roll(values, 96, 1), pltpu.roll(values, 32, 1))
        return values * cosine + swapped * sine

    for i in range(group):
        b = step * group + i
        ctx = ctx_ref[b]
        rows = slice(i * NODES, (i + 1) * NODES)
        position = depth_ref[i] + ctx
        hot = (lax.broadcasted_iota(jnp.int32, (SPAN, NODES), 0) == position).astype(F32).astype(BF16)
        looked = dot_tn(hot, table_ref[...])
        both = looked[:, :256] + looked[:, 256:512] + looked[:, 512:]
        cosine, sine = both[:, :128], both[:, 128:]
        q01 = (rope(q_all[rows, :128], cosine, sine) * 0.125).astype(BF16)
        q23 = (rope(q_all[rows, 128:], cosine, sine) * 0.125).astype(BF16)
        kv_new = rope(kv_all[rows], jnp.where(low, cosine, 1.0), jnp.where(low, sine, 0.0)).astype(BF16)
        for p in range(PAGES):
            old_ref[i, p * PAGE:(p + 1) * PAGE, :] = kv_ref[bt_ref[b, p]].astype(F32)
        slot = lax.broadcasted_iota(jnp.int32, (SPAN, NODES), 0)
        node = lax.broadcasted_iota(jnp.int32, (SPAN, NODES), 1)
        place = (slot - node == ctx).astype(F32).astype(BF16)
        shifted = dot(place, kv_new)
        slot_col = lax.broadcasted_iota(jnp.int32, (SPAN, 128), 0)
        fresh = (slot_col >= ctx) & (slot_col < ctx + NODES)
        merged = jnp.where(fresh, shifted, old_ref[i])
        merged16 = merged.astype(BF16)
        for p in range(PAGES):
            kvout_ref[bt_ref[b, p]] = merged16[p * PAGE:(p + 1) * PAGE]
        turned = pltpu.roll(merged, 64, 1)
        k_even = jnp.where(low, merged, 0.0).astype(BF16)
        v_odd = jnp.where(low, 0.0, merged).astype(BF16)
        v_even = jnp.where(low, turned, 0.0).astype(BF16)
        k_odd = jnp.where(low, 0.0, turned).astype(BF16)
        tree = dot_nt(mask_ref[i].astype(F32).astype(BF16), place)
        slot_row = lax.broadcasted_iota(jnp.int32, (NODES, SPAN), 1)
        seen = (slot_row < ctx) | (tree > 0.5)

        def head(query, keys):
            score = jnp.where(seen, dot_nt(query, keys), -jnp.inf)
            weight = jnp.exp(score - jnp.max(score, axis=-1, keepdims=True))
            return weight.astype(BF16), jnp.sum(weight, axis=-1, keepdims=True)

        for pair, query in enumerate((q01, q23)):
            w_even, t_even = head(query, k_even)
            w_odd, t_odd = head(query, k_odd)
            mixed = dot(w_even, v_even) + dot(w_odd, v_odd)
            att_ref[rows, pair * 128:(pair + 1) * 128] = (mixed / jnp.where(low, t_even, t_odd)).astype(BF16)


def attention(hidden, tree_mask, depth, ctx_len, block_table, kv_cache, attn_norm, w_q, w_k, w_v, table):
    group = 4
    grid = (hidden.shape[0] // (group * NODES),)
    spec = pltpu.PrefetchScalarGridSpec(
        num_scalar_prefetch=2,
        grid=grid,
        in_specs=[
            pl.BlockSpec((group * NODES, DIM), lambda i, *_: (i, 0)),
            pl.BlockSpec((group, 1, NODES), lambda i, *_: (i, 0, 0)),
            pl.BlockSpec((group, NODES, NODES), lambda i, *_: (i, 0, 0)),
            pl.BlockSpec((1, DIM), lambda i, *_: (0, 0)),
            pl.BlockSpec((DIM, 256), lambda i, *_: (0, 0)),
            pl.BlockSpec((HD, DIM), lambda i, *_: (0, 0)),
            pl.BlockSpec((HD, DIM), lambda i, *_: (0, 0)),
            pl.BlockSpec(table.shape, lambda i, *_: (0, 0)),
            pl.BlockSpec(kv_cache.shape, lambda i, *_: (0, 0, 0)),
        ],
        out_specs=[
            pl.BlockSpec((group * NODES, 256), lambda i, *_: (i, 0)),
            pl.BlockSpec(kv_cache.shape, lambda i, *_: (0, 0, 0)),
        ],
        scratch_shapes=[pltpu.VMEM((group, SPAN, 128), F32)],
    )
    return pl.pallas_call(
        functools.partial(attention_kernel, group),
        grid_spec=spec,
        out_shape=[jax.ShapeDtypeStruct((hidden.shape[0], 256), BF16), jax.ShapeDtypeStruct(kv_cache.shape, BF16)],
        compiler_params=pltpu.CompilerParams(vmem_limit_bytes=40 * 2**20),
        name="attention",
    )(ctx_len, block_table, hidden, depth, tree_mask, attn_norm, w_q, w_k, w_v, table, kv_cache)


def layer_kernel(att, wo, hid, mgain, wg_hbm, wu_hbm, wd_hbm, fgain, wlm, sid, ln_ref, lp_ref,
                 wg, wu, wd, wbuf, psib, pown, s1buf, s2buf, mfull, hown, pact, lg0, lg1, mrun, srun, prun, wanted, stat,
                 load_sem, tile_sem, s1_send, s1_recv, s2_send, s2_recv, ag_send, ag_recv, fw_send, fw_recv, fin_send, fin_recv):
    me = lax.axis_index("tp")
    core = me % 2
    chip = me // 2
    cx = chip % 2
    cy = chip // 2
    sib = me + 1 - 2 * core
    far = (chip + 1 - 2 * cx, chip + 2 - 4 * cy, 3 - chip)

    def peer(rel):
        return 2 * far[rel] + core

    def remote(src, dst, ssem, rsem, target):
        return pltpu.make_async_remote_copy(src_ref=src, dst_ref=dst, send_sem=ssem, recv_sem=rsem, device_id={"tp": target}, device_id_type=MESH)

    barrier = pltpu.get_barrier_semaphore()
    for off in range(1, 8):
        pl.semaphore_signal(barrier, inc=1, device_id={"tp": (me + off) % 8}, device_id_type=MESH)

    loads = [
        pltpu.make_async_copy(wg_hbm, wg, load_sem.at[0]),
        pltpu.make_async_copy(wu_hbm, wu, load_sem.at[1]),
        pltpu.make_async_copy(wd_hbm, wd, load_sem.at[2]),
    ]

    def own_rows(c):
        return c * CR + (core * 4 + chip) * BR

    hid_loads = [
        pltpu.make_async_copy(hid.at[pl.ds(pl.multiple_of(own_rows(c), BR), BR)], hown.at[pl.ds(c * BR, BR)], load_sem.at[3 + c])
        for c in range(CHUNKS)
    ]
    for copy in hid_loads + loads:
        copy.start()

    def tile_copy(t):
        first = jnp.minimum((t % TILES) * TILE, VOCAB - TILE)
        return pltpu.make_async_copy(wlm.at[pl.ds(pl.multiple_of(first, 16), TILE)], wbuf.at[t % 4], tile_sem.at[t % 4])

    tile_copy(0).start()
    tile_copy(1).start()

    mrun[...] = jnp.full_like(mrun, LOWEST)
    srun[...] = jnp.zeros_like(srun)
    prun[...] = jnp.zeros_like(prun)
    for i in range(16):
        wanted[:, pl.ds(i * NODES, NODES)] = sid[pl.ds(i, 1)] - me * VOCAB

    def half_rows(c, which):
        return pl.ds(pl.multiple_of(c * CR + which * HALF, HALF), HALF)

    def slab(c):
        return pl.ds(c * HALF, HALF)

    def first_copy(s, c):
        return remote(psib.at[s, slab(c)], s1buf.at[s, slab(c)], s1_send.at[s, c], s1_recv.at[s, c], sib)

    def project(c):
        psib[0, slab(c)] = dot(att[half_rows(c, 1 - core)], wo[...]).astype(BF16)
        if c == 0:
            pl.semaphore_wait(barrier, 7)
        first_copy(0, c).start()
        pown[0, slab(c)] = dot(att[half_rows(c, core)], wo[...]).astype(BF16)

    def second_copy(s, c, rel):
        block = pl.ds(pl.multiple_of(c * HALF + far[rel] * BR, BR), BR)
        return remote(pown.at[s, block], s2buf.at[s, c, rel], s2_send.at[s, c, rel], s2_recv.at[s, c, rel], peer(rel))

    def pair_sum(s, c):
        first_copy(s, c).wait_recv()
        pown[s, slab(c)] = (pown[s, slab(c)].astype(F32) + s1buf[s, slab(c)].astype(F32)).astype(BF16)
        for rel in range(3):
            second_copy(s, c, rel).start()

    def block_rows(c, k, q):
        return pl.ds(pl.multiple_of(c * CR + (k * 4 + q) * BR, BR), BR)

    def gather_copy(s, c, rel, rows):
        target = sib if rel == 3 else peer(rel)
        return remote(mfull.at[s, rows], mfull.at[s, rows], ag_send.at[s, c, rel], ag_recv.at[s, c, rel], target)

    def forward_copy(s, c, rel, rows):
        return remote(mfull.at[s, rows], mfull.at[s, rows], fw_send.at[s, c, rel], fw_recv.at[s, c, rel], sib)

    def finish_sum(s, c):
        for rel in range(3):
            second_copy(s, c, rel).wait_recv()
        total = pown[s, pl.ds(pl.multiple_of(c * HALF + chip * BR, BR), BR)].astype(F32)
        for rel in range(3):
            total = total + s2buf[s, c, rel].astype(F32)
        if s == 0:
            hid_loads[c].wait()
        rows = pl.ds(c * BR, BR)
        state = (hown[rows].astype(F32) + total.astype(BF16).astype(F32)).astype(BF16)
        if s == 0:
            hown[rows] = state
        gain = (mgain if s == 0 else fgain)[...].astype(F32)
        mine = block_rows(c, core, chip)
        mfull[s, mine] = normalize(state.astype(F32), gain)
        for rel in range(4):
            gather_copy(s, c, rel, mine).start()

    def forward(s, c):
        for rel in range(3):
            rows = block_rows(c, core, far[rel])
            gather_copy(s, c, rel, rows).wait_recv()
            forward_copy(s, c, rel, rows).start()

    def complete(s, c):
        gather_copy(s, c, 3, block_rows(c, 1 - core, chip)).wait_recv()
        for rel in range(3):
            forward_copy(s, c, rel, block_rows(c, 1 - core, far[rel])).wait_recv()

    def mlp(c):
        if c == 0:
            for copy in loads:
                copy.wait()

        def up(j, carry):
            cols = pl.ds(pl.multiple_of(j * 256, 256), 256)
            values = mfull[0, pl.ds(c * CR, CR)]
            gate = dot(values, wg[:, cols])
            upper = dot(values, wu[:, cols])
            pact[:, cols] = (gate * (1.0 / (1.0 + jnp.exp(-gate))) * upper).astype(BF16)
            return carry

        lax.fori_loop(0, FFN // 256, up, 0)

        def down(which, out):
            rows = pl.ds(pl.multiple_of(which * HALF, HALF), HALF)

            def one(j, carry):
                cols = pl.ds(pl.multiple_of(j * 512, 512), 512)
                out[1, slab(c), cols] = dot(pact[rows], wd[:, cols]).astype(BF16)
                return carry

            lax.fori_loop(0, DIM // 512, one, 0)

        down(1 - core, psib)
        first_copy(1, c).start()
        down(core, pown)

    def chunk_rows(t):
        return pl.ds(pl.multiple_of((t // TILES) * CR, CR), CR)

    def multiply(logits, t):
        logits[...] = dot_nt(wbuf[t % 4], mfull[1, chunk_rows(t)])

    def absorb(logits, t):
        j = (t + TILES) % TILES
        rows = chunk_rows(jnp.maximum(t, 0))
        last = j == TILES - 1
        blocks = []
        for g in range(TILE // 8):
            x = logits[g * 8:(g + 1) * 8, :]
            blocks.append(jnp.where(last, -jnp.inf, x) if g * 8 < REPEAT else x)
        first = jnp.where(t < 0, 2 * VOCAB * 8, jnp.minimum(j * TILE, VOCAB - TILE))
        offset = wanted[:, rows] - first - lax.broadcasted_iota(jnp.int32, (8, CR), 0)
        before = mrun[:, rows]
        tops = [before] + [None] * 3
        for g, x in enumerate(blocks):
            old = tops[g % 4]
            tops[g % 4] = x if old is None else jnp.maximum(old, x)
        top = jnp.maximum(jnp.maximum(tops[0], tops[1]), jnp.maximum(tops[2], tops[3]))
        totals = [srun[:, rows] * jnp.exp(before - top)] + [jnp.zeros_like(top)] * 3
        picked = [prun[:, rows]] + [jnp.zeros_like(top)] * 3
        for g, x in enumerate(blocks):
            totals[g % 4] = totals[g % 4] + jnp.exp(x - top)
            hit = offset == g * 8
            if g * 8 < REPEAT:
                hit = hit & jnp.logical_not(last)
            picked[g % 4] = picked[g % 4] + jnp.where(hit, x, 0.0)
        mrun[:, rows] = top
        srun[:, rows] = (totals[0] + totals[1]) + (totals[2] + totals[3])
        prun[:, rows] = (picked[0] + picked[1]) + (picked[2] + picked[3])

    def vocab(events):
        lg1[...] = jnp.full_like(lg1, LOWEST)

        def step(i, carry):
            t = 2 * i

            @pl.when(t + 2 < CHUNKS * TILES)
            def _():
                tile_copy(t + 2).start()
                tile_copy(t + 3).start()

            for at, event in events:
                pl.when(i == at)(event)
            tile_copy(t).wait()
            tile_copy(t + 1).wait()
            multiply(lg0, t)
            absorb(lg1, t - 1)
            multiply(lg1, t + 1)
            absorb(lg0, t)
            return carry

        lax.fori_loop(0, CHUNKS * TILES // 2, step, 0)
        absorb(lg1, CHUNKS * TILES - 1)

    project(0)
    project(1)
    pair_sum(0, 0)
    finish_sum(0, 0)
    pair_sum(0, 1)
    forward(0, 0)
    complete(0, 0)
    mlp(0)
    pair_sum(1, 0)
    finish_sum(0, 1)
    finish_sum(1, 0)
    forward(0, 1)
    complete(0, 1)
    mlp(1)
    forward(1, 0)
    complete(1, 0)
    vocab((
        (1, lambda: pair_sum(1, 1)),
        (4, lambda: finish_sum(1, 1)),
        (7, lambda: forward(1, 1)),
        (8, lambda: complete(1, 1)),
    ))

    tops = mrun[...]
    top = jnp.max(tops, axis=0, keepdims=True)
    stat[0, 0:1] = top
    stat[0, 1:2] = jnp.sum(srun[...] * jnp.exp(tops - top), axis=0, keepdims=True)
    stat[0, 2:3] = jnp.sum(prun[...], axis=0, keepdims=True)

    def stat_copy(off):
        return remote(stat.at[0], stat.at[off], fin_send.at[off - 1], fin_recv.at[off - 1], (me + off) % 8)

    for off in range(1, 8):
        stat_copy(off).start()
    for off in range(1, 8):
        stat_copy(off).wait_recv()
    top = stat[0, 0:1]
    for off in range(1, 8):
        top = jnp.maximum(top, stat[off, 0:1])
    total = jnp.zeros_like(top)
    picked = jnp.zeros_like(top)
    for off in range(8):
        total = total + stat[off, 1:2] * jnp.exp(stat[off, 0:1] - top)
        picked = picked + stat[off, 2:3]
    log_norm = top + jnp.log(total)
    log_prob = picked - log_norm
    for i in range(16):
        ln_ref[pl.ds(i, 1), :] = log_norm[:, i * NODES:(i + 1) * NODES]
        lp_ref[pl.ds(i, 1), :] = log_prob[:, i * NODES:(i + 1) * NODES]

    for s in range(2):
        for c in range(CHUNKS):
            first_copy(s, c).wait_send()
            mine = block_rows(c, core, chip)
            for rel in range(4):
                gather_copy(s, c, rel, mine).wait_send()
            for rel in range(3):
                second_copy(s, c, rel).wait_send()
                forward_copy(s, c, rel, block_rows(c, core, far[rel])).wait_send()
    for off in range(1, 8):
        stat_copy(off).wait_send()


def layer(att, w_o, hidden, mlp_norm, w_gate, w_up, w_down, final_norm, w_lm, score_id):
    vmem = pl.BlockSpec(memory_space=pltpu.VMEM)
    hbm = pl.BlockSpec(memory_space=pl.ANY)
    sem = pltpu.SemaphoreType.DMA
    return pl.pallas_call(
        layer_kernel,
        in_specs=[vmem, vmem, hbm, vmem, hbm, hbm, hbm, vmem, hbm, vmem],
        out_specs=[vmem, vmem],
        out_shape=[jax.ShapeDtypeStruct((16, NODES), F32)] * 2,
        scratch_shapes=[
            pltpu.VMEM((DIM, FFN), BF16),
            pltpu.VMEM((DIM, FFN), BF16),
            pltpu.VMEM((FFN, DIM), BF16),
            pltpu.VMEM((4, TILE, DIM), BF16),
            pltpu.VMEM((2, ROWS // 2, DIM), BF16),
            pltpu.VMEM((2, ROWS // 2, DIM), BF16),
            pltpu.VMEM((2, ROWS // 2, DIM), BF16),
            pltpu.VMEM((2, CHUNKS, 3, BR, DIM), BF16),
            pltpu.VMEM((2, ROWS, DIM), BF16),
            pltpu.VMEM((ROWS // 8, DIM), BF16),
            pltpu.VMEM((CR, FFN), BF16),
            pltpu.VMEM((TILE, CR), F32),
            pltpu.VMEM((TILE, CR), F32),
            pltpu.VMEM((8, ROWS), F32),
            pltpu.VMEM((8, ROWS), F32),
            pltpu.VMEM((8, ROWS), F32),
            pltpu.VMEM((1, ROWS), jnp.int32),
            pltpu.VMEM((8, 8, ROWS), F32),
            sem((3 + CHUNKS,)),
            sem((4,)),
            sem((2, CHUNKS)),
            sem((2, CHUNKS)),
            sem((2, CHUNKS, 3)),
            sem((2, CHUNKS, 3)),
            sem((2, CHUNKS, 4)),
            sem((2, CHUNKS, 4)),
            sem((2, CHUNKS, 3)),
            sem((2, CHUNKS, 3)),
            sem((7,)),
            sem((7,)),
        ],
        compiler_params=pltpu.CompilerParams(collective_id=0, has_side_effects=True, vmem_limit_bytes=63 * 2**20),
        name="layer",
    )(att, w_o, hidden, mlp_norm, w_gate, w_up, w_down, final_norm, w_lm, score_id)


def solution(mesh):
    def group_step(hidden, tree_mask, depth, ctx_len, block_table, score_id, k_cache, v_cache, attn_norm, w_q, w_k, w_v, w_o, mlp_norm, w_gate, w_up, w_down, final_norm, w_lm):
        flat = hidden.reshape(ROWS, DIM)
        kv_cache = jnp.concatenate([k_cache[:, :, 0], v_cache[:, :, 0]], axis=-1)
        table = jnp.asarray(rope_table())
        att, kv_out = attention(flat, tree_mask, depth[:, None, :], ctx_len, block_table, kv_cache, attn_norm[None], w_q, w_k.T, w_v.T, table)
        log_norm, log_prob = layer(att, w_o, flat, mlp_norm[None], w_gate, w_up, w_down, final_norm[None], w_lm.T, score_id)
        return log_norm, log_prob, kv_out[:, :, None, :HD], kv_out[:, :, None, HD:]

    request_spec = P("dp", None, None)
    node_spec = P("dp", None)
    cache_spec = P("dp", None, "tp", None)
    shared_spec = P(None)
    column_spec = P(None, "tp")
    row_spec = P("tp", None)
    in_specs = (request_spec, request_spec, node_spec, P("dp"), node_spec, node_spec, cache_spec, cache_spec, shared_spec, column_spec, column_spec, column_spec, row_spec, shared_spec, column_spec, column_spec, row_spec, shared_spec, column_spec)
    out_specs = (node_spec, node_spec, cache_spec, cache_spec)
    return jax.shard_map(group_step, mesh=mesh, in_specs=in_specs, out_specs=out_specs, check_vma=False)
```

```python
import functools

import jax
import jax.numpy as jnp
import numpy as np
from jax import lax
from jax.experimental import pallas as pl
from jax.experimental.pallas import tpu as pltpu
from jax.sharding import PartitionSpec as P

RMS_EPS = 1e-5
ROPE_THETA = 500000
DIM = 2048
ROWS = 1024
NODES = 64
PAGES = 12
PAGE = 16
SPAN = PAGES * PAGE
HD = 64
FFN = 1024
VOCAB = 16032
TILE = 1008
TILES = 16
REPEAT = TILES * TILE - VOCAB
LOWEST = -3e38
CHUNKS = 4
PASSES = 2
PR = ROWS // PASSES
HD_COLS = DIM // 2
CR = ROWS // CHUNKS
HALF = CR // 2
BR = CR // 8
MESH = pl.DeviceIdType.MESH
F32 = jnp.float32
BF16 = jnp.bfloat16


BEFORE = "O0 O1 A00 A01 R00 R01 B00 B01 O2 O3 F00 A02 F01 C00 M0 C01 A10 M1 A11 R02 R10 B10 R11 B11 F10 F11 C10 C11"
DURING = ("B02 A03", "R03 F02", "B03 C02 M2", "F03 A12 C03 M3", "R12 A13", "B12 R13", "B13 F12", "C12 F13", "C13")


def rope_table():
    half = HD // 2
    freq = (np.float32(1.0) / np.power(np.float32(ROPE_THETA), np.arange(half, dtype=np.float32) * np.float32(2.0 / HD))).astype(np.float32)
    angle = (np.arange(SPAN, dtype=np.float32)[:, None] * freq[None, :]).astype(np.float32).astype(np.float64)
    cos = np.tile(np.cos(angle), (1, 4)).astype(np.float32)
    sin = np.sin(angle)
    sin = np.concatenate([-sin, sin, -sin, sin], axis=1).astype(np.float32)
    table = np.concatenate([cos, sin], axis=1)
    high = table.astype(jnp.bfloat16)
    rest = table - high.astype(np.float32)
    mid = rest.astype(jnp.bfloat16)
    low = (rest - mid.astype(np.float32)).astype(jnp.bfloat16)
    return np.concatenate([high, mid, low], axis=1)


def normalize(values, gain):
    scale = lax.rsqrt(jnp.mean(values * values, axis=-1, keepdims=True) + RMS_EPS)
    return (values * scale * gain).astype(BF16)


def dot(a, b):
    return jnp.dot(a, b, preferred_element_type=F32)


def dot_nt(a, b):
    return lax.dot_general(a, b, (((1,), (1,)), ((), ())), preferred_element_type=F32)


def dot_tn(a, b):
    return lax.dot_general(a, b, (((0,), (0,)), ((), ())), preferred_element_type=F32)


def attention_kernel(group, ctx_ref, bt_ref, hid_ref, depth_ref, mask_ref, gain_ref, wq_ref, wk_ref, wv_ref, table_ref, kv_ref, att_ref, kvout_ref, old_ref):
    step = pl.program_id(0)
    normed = normalize(hid_ref[...].astype(F32), gain_ref[...].astype(F32))
    q_all = dot(normed, wq_ref[...])
    kv_all = dot_nt(normed, jnp.concatenate([wk_ref[...], wv_ref[...]], axis=0))
    lane = lax.broadcasted_iota(jnp.int32, (1, 128), 1)
    low = lane < 64
    first = (lane % 64) < 32

    def rope(values, cosine, sine):
        swapped = jnp.where(first, pltpu.roll(values, 96, 1), pltpu.roll(values, 32, 1))
        return values * cosine + swapped * sine

    for i in range(group):
        b = step * group + i
        ctx = ctx_ref[b]
        rows = slice(i * NODES, (i + 1) * NODES)
        position = depth_ref[i] + ctx
        hot = (lax.broadcasted_iota(jnp.int32, (SPAN, NODES), 0) == position).astype(F32).astype(BF16)
        looked = dot_tn(hot, table_ref[...])
        both = looked[:, :256] + looked[:, 256:512] + looked[:, 512:]
        cosine, sine = both[:, :128], both[:, 128:]
        q01 = (rope(q_all[rows, :128], cosine, sine) * 0.125).astype(BF16)
        q23 = (rope(q_all[rows, 128:], cosine, sine) * 0.125).astype(BF16)
        kv_new = rope(kv_all[rows], jnp.where(low, cosine, 1.0), jnp.where(low, sine, 0.0)).astype(BF16)
        for p in range(PAGES):
            old_ref[i, p * PAGE:(p + 1) * PAGE, :] = kv_ref[bt_ref[b, p]].astype(F32)
        slot = lax.broadcasted_iota(jnp.int32, (SPAN, NODES), 0)
        node = lax.broadcasted_iota(jnp.int32, (SPAN, NODES), 1)
        place = (slot - node == ctx).astype(F32).astype(BF16)
        shifted = dot(place, kv_new)
        slot_col = lax.broadcasted_iota(jnp.int32, (SPAN, 128), 0)
        fresh = (slot_col >= ctx) & (slot_col < ctx + NODES)
        merged = jnp.where(fresh, shifted, old_ref[i])
        merged16 = merged.astype(BF16)
        for p in range(PAGES):
            kvout_ref[bt_ref[b, p]] = merged16[p * PAGE:(p + 1) * PAGE]
        turned = pltpu.roll(merged, 64, 1)
        k_even = jnp.where(low, merged, 0.0).astype(BF16)
        v_odd = jnp.where(low, 0.0, merged).astype(BF16)
        v_even = jnp.where(low, turned, 0.0).astype(BF16)
        k_odd = jnp.where(low, 0.0, turned).astype(BF16)
        tree = dot_nt(mask_ref[i].astype(F32).astype(BF16), place)
        slot_row = lax.broadcasted_iota(jnp.int32, (NODES, SPAN), 1)
        seen = (slot_row < ctx) | (tree > 0.5)

        def head(query, keys):
            score = jnp.where(seen, dot_nt(query, keys), -jnp.inf)
            weight = jnp.exp(score - jnp.max(score, axis=-1, keepdims=True))
            return weight.astype(BF16), jnp.sum(weight, axis=-1, keepdims=True)

        for pair, query in enumerate((q01, q23)):
            w_even, t_even = head(query, k_even)
            w_odd, t_odd = head(query, k_odd)
            mixed = dot(w_even, v_even) + dot(w_odd, v_odd)
            att_ref[rows, pair * 128:(pair + 1) * 128] = (mixed / jnp.where(low, t_even, t_odd)).astype(BF16)


def attention(hidden, tree_mask, depth, ctx_len, block_table, kv_cache, attn_norm, w_q, w_k, w_v, table):
    group = 4
    grid = (hidden.shape[0] // (group * NODES),)
    spec = pltpu.PrefetchScalarGridSpec(
        num_scalar_prefetch=2,
        grid=grid,
        in_specs=[
            pl.BlockSpec((group * NODES, DIM), lambda i, *_: (i, 0)),
            pl.BlockSpec((group, 1, NODES), lambda i, *_: (i, 0, 0)),
            pl.BlockSpec((group, NODES, NODES), lambda i, *_: (i, 0, 0)),
            pl.BlockSpec((1, DIM), lambda i, *_: (0, 0)),
            pl.BlockSpec((DIM, 256), lambda i, *_: (0, 0)),
            pl.BlockSpec((HD, DIM), lambda i, *_: (0, 0)),
            pl.BlockSpec((HD, DIM), lambda i, *_: (0, 0)),
            pl.BlockSpec(table.shape, lambda i, *_: (0, 0)),
            pl.BlockSpec(kv_cache.shape, lambda i, *_: (0, 0, 0)),
        ],
        out_specs=[
            pl.BlockSpec((group * NODES, 256), lambda i, *_: (i, 0)),
            pl.BlockSpec(kv_cache.shape, lambda i, *_: (0, 0, 0)),
        ],
        scratch_shapes=[pltpu.VMEM((group, SPAN, 128), F32)],
    )
    return pl.pallas_call(
        functools.partial(attention_kernel, group),
        grid_spec=spec,
        out_shape=[jax.ShapeDtypeStruct((hidden.shape[0], 256), BF16), jax.ShapeDtypeStruct(kv_cache.shape, BF16)],
        compiler_params=pltpu.CompilerParams(vmem_limit_bytes=40 * 2**20),
        name="attention",
    )(ctx_len, block_table, hidden, depth, tree_mask, attn_norm, w_q, w_k, w_v, table, kv_cache)


def layer_kernel(att, wo, hid, mgain, wg_hbm, wu_hbm, wd_hbm, fgain, wlm, sid, ln_ref, lp_ref,
                 wg, wu, wd, wbuf, psib, pown, s1buf, s2buf, mfull, hown, pact, lg0, lg1, mrun, srun, prun, wanted, stat,
                 load_sem, tile_sem, s1_send, s1_recv, s2_send, s2_recv, ag_send, ag_recv, fw_send, fw_recv, cr_send, cr_recv, fin_send, fin_recv):
    me = lax.axis_index("tp")
    core = me % 2
    chip = me // 2
    cx = chip % 2
    cy = chip // 2
    sib = me + 1 - 2 * core
    far = (chip + 1 - 2 * cx, chip + 2 - 4 * cy, 3 - chip)

    def peer(rel):
        return 2 * far[rel] + core

    def remote(src, dst, ssem, rsem, target):
        return pltpu.make_async_remote_copy(src_ref=src, dst_ref=dst, send_sem=ssem, recv_sem=rsem, device_id={"tp": target}, device_id_type=MESH)

    barrier = pltpu.get_barrier_semaphore()
    for off in range(1, 8):
        pl.semaphore_signal(barrier, inc=1, device_id={"tp": (me + off) % 8}, device_id_type=MESH)

    loads = [
        pltpu.make_async_copy(wg_hbm, wg, load_sem.at[0]),
        pltpu.make_async_copy(wu_hbm, wu, load_sem.at[1]),
        pltpu.make_async_copy(wd_hbm, wd, load_sem.at[2]),
    ]

    def own_rows(c):
        return c * CR + (core * 4 + chip) * BR

    hid_loads = [
        pltpu.make_async_copy(hid.at[pl.ds(pl.multiple_of(own_rows(c), BR), BR)], hown.at[pl.ds(c * BR, BR)], load_sem.at[3 + c])
        for c in range(CHUNKS)
    ]
    for copy in hid_loads + loads:
        copy.start()

    def tile_copy(t):
        first = jnp.minimum((t % TILES) * TILE, VOCAB - TILE)
        return pltpu.make_async_copy(wlm.at[pl.ds(pl.multiple_of(first, 16), TILE)], wbuf.at[t % 4], tile_sem.at[t % 4])

    tile_copy(0).start()
    tile_copy(1).start()

    mrun[...] = jnp.full_like(mrun, LOWEST)
    srun[...] = jnp.zeros_like(srun)
    prun[...] = jnp.zeros_like(prun)
    for i in range(16):
        wanted[:, pl.ds(i * NODES, NODES)] = sid[pl.ds(i, 1)] - me * VOCAB

    def half_rows(c, which):
        return pl.ds(pl.multiple_of(c * CR + which * HALF, HALF), HALF)

    def slab(c):
        return pl.ds(c * HALF, HALF)

    def first_copy(s, c):
        return remote(psib.at[s, slab(c)], s1buf.at[s, slab(c)], s1_send.at[s, c], s1_recv.at[s, c], sib)

    def project(c):
        psib[0, slab(c)] = dot(att[half_rows(c, 1 - core)], wo[...]).astype(BF16)
        if c == 0:
            pl.semaphore_wait(barrier, 7)
        first_copy(0, c).start()
        pown[0, slab(c)] = dot(att[half_rows(c, core)], wo[...]).astype(BF16)

    first_cols = pl.ds(0, HD_COLS)
    last_cols = pl.ds(HD_COLS, HD_COLS)

    def stored(c, q):
        return pl.ds(pl.multiple_of(c * HALF + q * BR, BR), BR)

    def second_copy(s, c, i):
        q = (far[0], far[2], far[1], far[2], far[1], far[0])[i]
        target = peer((0, 0, 1, 1, 1, 0)[i])
        cols = (first_cols, first_cols, last_cols, last_cols, first_cols, last_cols)[i]
        return remote(pown.at[s, stored(c, q), cols], s2buf.at[s, c, i], s2_send.at[s, c, i], s2_recv.at[s, c, i], target)

    def pair_sum(s, c):
        first_copy(s, c).wait_recv()
        pown[s, slab(c)] = (pown[s, slab(c)].astype(F32) + s1buf[s, slab(c)].astype(F32)).astype(BF16)
        for i in (1, 3, 0, 2):
            second_copy(s, c, i).start()

    def relay(s, c):
        for i, q, cols in ((1, far[1], first_cols), (3, far[0], last_cols)):
            second_copy(s, c, i).wait_recv()
            rows = stored(c, q)
            pown[s, rows, cols] = (pown[s, rows, cols].astype(F32) + s2buf[s, c, i].astype(F32)).astype(BF16)
        for i in (4, 5):
            second_copy(s, c, i).start()

    def block_rows(c, k, q):
        return pl.ds(pl.multiple_of(c * CR + (k * 4 + q) * BR, BR), BR)

    def gather_copy(s, c, rel, rows):
        target = sib if rel == 3 else peer(rel)
        return remote(mfull.at[s, rows], mfull.at[s, rows], ag_send.at[s, c, rel], ag_recv.at[s, c, rel], target)

    def forward_copy(s, c, rel, rows):
        return remote(mfull.at[s, rows], mfull.at[s, rows], fw_send.at[s, c, rel], fw_recv.at[s, c, rel], sib)

    def finish_sum(s, c):
        for i in (0, 2, 4, 5):
            second_copy(s, c, i).wait_recv()
        rows = stored(c, chip)
        left = pown[s, rows, first_cols].astype(F32) + s2buf[s, c, 0].astype(F32) + s2buf[s, c, 4].astype(F32)
        right = pown[s, rows, last_cols].astype(F32) + s2buf[s, c, 2].astype(F32) + s2buf[s, c, 5].astype(F32)
        total = jnp.concatenate([left, right], axis=1)
        if s == 0:
            hid_loads[c].wait()
        rows = pl.ds(c * BR, BR)
        state = (hown[rows].astype(F32) + total.astype(BF16).astype(F32)).astype(BF16)
        if s == 0:
            hown[rows] = state
        gain = (mgain if s == 0 else fgain)[...].astype(F32)
        mine = block_rows(c, core, chip)
        mfull[s, mine] = normalize(state.astype(F32), gain)
        for rel in (0, 1, 3):
            gather_copy(s, c, rel, mine).start()

    def cross_copy(s, c, i, q):
        rows = block_rows(c, core, q)
        cols = (last_cols, first_cols)[i]
        part = mfull.at[s, rows, cols]
        return remote(part, part, cr_send.at[s, c, i], cr_recv.at[s, c, i], peer(1 - i))

    def forward(s, c):
        for rel in range(2):
            rows = block_rows(c, core, far[rel])
            gather_copy(s, c, rel, rows).wait_recv()
            cross_copy(s, c, rel, far[rel]).start()
            forward_copy(s, c, rel, rows).start()

    def complete(s, c):
        for i in range(2):
            cross_copy(s, c, i, far[2]).wait_recv()
        forward_copy(s, c, 2, block_rows(c, core, far[2])).start()
        gather_copy(s, c, 3, block_rows(c, 1 - core, chip)).wait_recv()
        for rel in range(3):
            forward_copy(s, c, rel, block_rows(c, 1 - core, far[rel])).wait_recv()

    def mlp(c):
        if c == 0:
            for copy in loads:
                copy.wait()

        def up(j, carry):
            cols = pl.ds(pl.multiple_of(j * 256, 256), 256)
            values = mfull[0, pl.ds(c * CR, CR)]
            gate = dot(values, wg[:, cols])
            upper = dot(values, wu[:, cols])
            pact[:, cols] = (gate * (1.0 / (1.0 + jnp.exp(-gate))) * upper).astype(BF16)
            return carry

        lax.fori_loop(0, FFN // 256, up, 0)

        def down(which, out):
            rows = pl.ds(pl.multiple_of(which * HALF, HALF), HALF)

            def one(j, carry):
                cols = pl.ds(pl.multiple_of(j * 512, 512), 512)
                out[1, slab(c), cols] = dot(pact[rows], wd[:, cols]).astype(BF16)
                return carry

            lax.fori_loop(0, DIM // 512, one, 0)

        down(1 - core, psib)
        first_copy(1, c).start()
        down(core, pown)

    def chunk_rows(t):
        return pl.ds(pl.multiple_of((t // TILES) * PR, PR), PR)

    def multiply(logits, t):
        for part in range(2):
            piece = slice(part * TILE // 2, (part + 1) * TILE // 2)
            logits[piece, :] = dot_nt(wbuf[t % 4, piece], mfull[1, chunk_rows(t)])

    def absorb(logits, t):
        j = (t + TILES) % TILES
        rows = chunk_rows(jnp.maximum(t, 0))
        last = j == TILES - 1
        blocks = []
        for g in range(TILE // 8):
            x = logits[g * 8:(g + 1) * 8, :]
            blocks.append(jnp.where(last, -jnp.inf, x) if g * 8 < REPEAT else x)
        first = jnp.where(t < 0, 2 * VOCAB * 8, jnp.minimum(j * TILE, VOCAB - TILE))
        offset = wanted[:, rows] - first - lax.broadcasted_iota(jnp.int32, (8, PR), 0)
        before = mrun[:, rows]
        tops = [before] + [None] * 3
        for g, x in enumerate(blocks):
            old = tops[g % 4]
            tops[g % 4] = x if old is None else jnp.maximum(old, x)
        top = jnp.maximum(jnp.maximum(tops[0], tops[1]), jnp.maximum(tops[2], tops[3]))
        totals = [srun[:, rows] * jnp.exp(before - top)] + [jnp.zeros_like(top)] * 3
        picked = [prun[:, rows]] + [jnp.zeros_like(top)] * 3
        for g, x in enumerate(blocks):
            totals[g % 4] = totals[g % 4] + jnp.exp(x - top)
            hit = offset == g * 8
            if g * 8 < REPEAT:
                hit = hit & jnp.logical_not(last)
            picked[g % 4] = picked[g % 4] + jnp.where(hit, x, 0.0)
        mrun[:, rows] = top
        srun[:, rows] = (totals[0] + totals[1]) + (totals[2] + totals[3])
        prun[:, rows] = (picked[0] + picked[1]) + (picked[2] + picked[3])

    def vocab(events):
        lg1[...] = jnp.full_like(lg1, LOWEST)

        def step(i, carry):
            t = 2 * i

            @pl.when(t + 2 < PASSES * TILES)
            def _():
                tile_copy(t + 2).start()
                tile_copy(t + 3).start()

            for at, event in events:
                pl.when(i == at)(event)
            tile_copy(t).wait()
            tile_copy(t + 1).wait()
            multiply(lg0, t)
            absorb(lg1, t - 1)
            multiply(lg1, t + 1)
            absorb(lg0, t)
            return carry

        lax.fori_loop(0, PASSES * TILES // 2, step, 0)
        absorb(lg1, PASSES * TILES - 1)

    acts = {"O": project, "A": pair_sum, "R": relay, "B": finish_sum, "F": forward, "C": complete, "M": mlp}

    def run(plan):
        for name in plan.split():
            if len(name) == 2:
                acts[name[0]](int(name[1]))
            else:
                acts[name[0]](int(name[1]), int(name[2]))

    run(BEFORE)
    vocab([(at, functools.partial(run, plan)) for at, plan in enumerate(DURING)])

    tops = mrun[...]
    top = jnp.max(tops, axis=0, keepdims=True)
    stat[0, 0:1] = top
    stat[0, 1:2] = jnp.sum(srun[...] * jnp.exp(tops - top), axis=0, keepdims=True)
    stat[0, 2:3] = jnp.sum(prun[...], axis=0, keepdims=True)

    def stat_copy(off):
        return remote(stat.at[0], stat.at[off], fin_send.at[off - 1], fin_recv.at[off - 1], (me + off) % 8)

    for off in range(1, 8):
        stat_copy(off).start()
    for off in range(1, 8):
        stat_copy(off).wait_recv()
    top = stat[0, 0:1]
    for off in range(1, 8):
        top = jnp.maximum(top, stat[off, 0:1])
    total = jnp.zeros_like(top)
    picked = jnp.zeros_like(top)
    for off in range(8):
        total = total + stat[off, 1:2] * jnp.exp(stat[off, 0:1] - top)
        picked = picked + stat[off, 2:3]
    log_norm = top + jnp.log(total)
    log_prob = picked - log_norm
    for i in range(16):
        ln_ref[pl.ds(i, 1), :] = log_norm[:, i * NODES:(i + 1) * NODES]
        lp_ref[pl.ds(i, 1), :] = log_prob[:, i * NODES:(i + 1) * NODES]

    for s in range(2):
        for c in range(CHUNKS):
            first_copy(s, c).wait_send()
            mine = block_rows(c, core, chip)
            for rel in (0, 1, 3):
                gather_copy(s, c, rel, mine).wait_send()
            for i in range(6):
                second_copy(s, c, i).wait_send()
            for rel in range(2):
                cross_copy(s, c, rel, far[rel]).wait_send()
            for rel in range(3):
                forward_copy(s, c, rel, block_rows(c, core, far[rel])).wait_send()
    for off in range(1, 8):
        stat_copy(off).wait_send()


def layer(att, w_o, hidden, mlp_norm, w_gate, w_up, w_down, final_norm, w_lm, score_id):
    vmem = pl.BlockSpec(memory_space=pltpu.VMEM)
    hbm = pl.BlockSpec(memory_space=pl.ANY)
    sem = pltpu.SemaphoreType.DMA
    return pl.pallas_call(
        layer_kernel,
        in_specs=[vmem, vmem, hbm, vmem, hbm, hbm, hbm, vmem, hbm, vmem],
        out_specs=[vmem, vmem],
        out_shape=[jax.ShapeDtypeStruct((16, NODES), F32)] * 2,
        scratch_shapes=[
            pltpu.VMEM((DIM, FFN), BF16),
            pltpu.VMEM((DIM, FFN), BF16),
            pltpu.VMEM((FFN, DIM), BF16),
            pltpu.VMEM((4, TILE, DIM), BF16),
            pltpu.VMEM((2, ROWS // 2, DIM), BF16),
            pltpu.VMEM((2, ROWS // 2, DIM), BF16),
            pltpu.VMEM((2, ROWS // 2, DIM), BF16),
            pltpu.VMEM((2, CHUNKS, 6, BR, HD_COLS), BF16),
            pltpu.VMEM((2, ROWS, DIM), BF16),
            pltpu.VMEM((ROWS // 8, DIM), BF16),
            pltpu.VMEM((CR, FFN), BF16),
            pltpu.VMEM((TILE, PR), F32),
            pltpu.VMEM((TILE, PR), F32),
            pltpu.VMEM((8, ROWS), F32),
            pltpu.VMEM((8, ROWS), F32),
            pltpu.VMEM((8, ROWS), F32),
            pltpu.VMEM((1, ROWS), jnp.int32),
            pltpu.VMEM((8, 8, ROWS), F32),
            sem((3 + CHUNKS,)),
            sem((4,)),
            sem((2, CHUNKS)),
            sem((2, CHUNKS)),
            sem((2, CHUNKS, 6)),
            sem((2, CHUNKS, 6)),
            sem((2, CHUNKS, 4)),
            sem((2, CHUNKS, 4)),
            sem((2, CHUNKS, 3)),
            sem((2, CHUNKS, 3)),
            sem((2, CHUNKS, 2)),
            sem((2, CHUNKS, 2)),
            sem((7,)),
            sem((7,)),
        ],
        compiler_params=pltpu.CompilerParams(collective_id=0, has_side_effects=True, vmem_limit_bytes=63 * 2**20),
        name="layer",
    )(att, w_o, hidden, mlp_norm, w_gate, w_up, w_down, final_norm, w_lm, score_id)


def solution(mesh):
    def group_step(hidden, tree_mask, depth, ctx_len, block_table, score_id, k_cache, v_cache, attn_norm, w_q, w_k, w_v, w_o, mlp_norm, w_gate, w_up, w_down, final_norm, w_lm):
        flat = hidden.reshape(ROWS, DIM)
        kv_cache = jnp.concatenate([k_cache[:, :, 0], v_cache[:, :, 0]], axis=-1)
        table = jnp.asarray(rope_table())
        att, kv_out = attention(flat, tree_mask, depth[:, None, :], ctx_len, block_table, kv_cache, attn_norm[None], w_q, w_k.T, w_v.T, table)
        log_norm, log_prob = layer(att, w_o, flat, mlp_norm[None], w_gate, w_up, w_down, final_norm[None], w_lm.T, score_id)
        return log_norm, log_prob, kv_out[:, :, None, :HD], kv_out[:, :, None, HD:]

    request_spec = P("dp", None, None)
    node_spec = P("dp", None)
    cache_spec = P("dp", None, "tp", None)
    shared_spec = P(None)
    column_spec = P(None, "tp")
    row_spec = P("tp", None)
    in_specs = (request_spec, request_spec, node_spec, P("dp"), node_spec, node_spec, cache_spec, cache_spec, shared_spec, column_spec, column_spec, column_spec, row_spec, shared_spec, column_spec, column_spec, row_spec, shared_spec, column_spec)
    out_specs = (node_spec, node_spec, cache_spec, cache_spec)
    return jax.shard_map(group_step, mesh=mesh, in_specs=in_specs, out_specs=out_specs, check_vma=False)
```

```python
import functools

import jax
import jax.numpy as jnp
import numpy as np
from jax import lax
from jax.experimental import pallas as pl
from jax.experimental.pallas import tpu as pltpu
from jax.sharding import PartitionSpec as P

RMS_EPS = 1e-5
ROPE_THETA = 500000
DIM = 2048
ROWS = 1024
NODES = 64
PAGES = 12
PAGE = 16
SPAN = PAGES * PAGE
HD = 64
FFN = 1024
VOCAB = 16032
TILE = 1008
TILES = 16
REPEAT = TILES * TILE - VOCAB
LOWEST = -3e38
CHUNKS = 4
PASSES = 2
PR = ROWS // PASSES
HD_COLS = DIM // 2
CR = ROWS // CHUNKS
HALF = CR // 2
BR = CR // 8
MESH = pl.DeviceIdType.MESH
F32 = jnp.float32
BF16 = jnp.bfloat16


BEFORE = "G T0 T1 O0 T2 A00 T3 O1 T4 A01 R00 T5 B00 R01 T6 B01 T7 O2 O3 F00 A02 F01 S C00 M0 C01 A10 M1 A11 R02 R10 B10 R11 B11 F10 F11 C10 C11"
DURING = ("B02 A03", "R03 F02", "B03 C02 M2", "F03 A12 C03 M3", "R12 A13", "B12 R13", "B13 F12", "C12 F13", "C13")


def rope_table():
    half = HD // 2
    freq = (np.float32(1.0) / np.power(np.float32(ROPE_THETA), np.arange(half, dtype=np.float32) * np.float32(2.0 / HD))).astype(np.float32)
    angle = (np.arange(SPAN, dtype=np.float32)[:, None] * freq[None, :]).astype(np.float32).astype(np.float64)
    cos = np.tile(np.cos(angle), (1, 4)).astype(np.float32)
    sin = np.sin(angle)
    sin = np.concatenate([-sin, sin, -sin, sin], axis=1).astype(np.float32)
    table = np.concatenate([cos, sin], axis=1)
    high = table.astype(jnp.bfloat16)
    rest = table - high.astype(np.float32)
    mid = rest.astype(jnp.bfloat16)
    low = (rest - mid.astype(np.float32)).astype(jnp.bfloat16)
    return np.concatenate([high, mid, low], axis=1)


def normalize(values, gain):
    scale = lax.rsqrt(jnp.mean(values * values, axis=-1, keepdims=True) + RMS_EPS)
    return (values * scale * gain).astype(BF16)


def dot(a, b):
    return jnp.dot(a, b, preferred_element_type=F32)


def dot_nt(a, b):
    return lax.dot_general(a, b, (((1,), (1,)), ((), ())), preferred_element_type=F32)


def dot_tn(a, b):
    return lax.dot_general(a, b, (((0,), (0,)), ((), ())), preferred_element_type=F32)


def layer_kernel(ctx_ref, hid, depth, mask, table_bt, sid, kc, vc, again, wq, wk, wv, table, wo, mgain, wg_hbm, wu_hbm, wd_hbm, fgain, wlm,
                 ln_ref, lp_ref, kc_out, vc_out,
                 att, pages, gk, gv, wg, wu, wd, wbuf, psib, pown, s1buf, s2buf, mfull, hown, pact, lg0, lg1, mrun, srun, prun, wanted, stat,
                 load_sem, tile_sem, s1_send, s1_recv, s2_send, s2_recv, ag_send, ag_recv, fw_send, fw_recv, cr_send, cr_recv, fin_send, fin_recv):
    me = lax.axis_index("tp")
    core = me % 2
    chip = me // 2
    cx = chip % 2
    cy = chip // 2
    sib = me + 1 - 2 * core
    far = (chip + 1 - 2 * cx, chip + 2 - 4 * cy, 3 - chip)

    def peer(rel):
        return 2 * far[rel] + core

    def remote(src, dst, ssem, rsem, target):
        return pltpu.make_async_remote_copy(src_ref=src, dst_ref=dst, send_sem=ssem, recv_sem=rsem, device_id={"tp": target}, device_id_type=MESH)

    barrier = pltpu.get_barrier_semaphore()
    for off in range(1, 8):
        pl.semaphore_signal(barrier, inc=1, device_id={"tp": (me + off) % 8}, device_id_type=MESH)

    loads = [
        pltpu.make_async_copy(wg_hbm, wg, load_sem.at[0]),
        pltpu.make_async_copy(wu_hbm, wu, load_sem.at[1]),
        pltpu.make_async_copy(wd_hbm, wd, load_sem.at[2]),
    ]

    def own_rows(c):
        return c * CR + (core * 4 + chip) * BR

    hid_loads = [
        pltpu.make_async_copy(hid.at[pl.ds(pl.multiple_of(own_rows(c), BR), BR)], hown.at[pl.ds(c * BR, BR)], load_sem.at[3 + c])
        for c in range(CHUNKS)
    ]
    half_loads = [
        pltpu.make_async_copy(hid.at[pl.ds(h * PR, PR)], wbuf.at[2 + h, pl.ds(0, PR)], load_sem.at[3 + CHUNKS + h])
        for h in range(2)
    ]
    for copy in half_loads + hid_loads + loads:
        copy.start()

    def tile_copy(t):
        first = jnp.minimum((t % TILES) * TILE, VOCAB - TILE)
        return pltpu.make_async_copy(wlm.at[pl.ds(pl.multiple_of(first, 16), TILE)], wbuf.at[t % 4], tile_sem.at[t % 4])

    tile_copy(0).start()
    tile_copy(1).start()

    mrun[...] = jnp.full_like(mrun, LOWEST)
    srun[...] = jnp.zeros_like(srun)
    prun[...] = jnp.zeros_like(prun)
    for i in range(16):
        wanted[:, pl.ds(i * NODES, NODES)] = sid[pl.ds(i, 1)] - me * VOCAB

    lane = lax.broadcasted_iota(jnp.int32, (1, 128), 1)
    low = lane < HD
    first_half = (lane % HD) < HD // 2

    def slot_of(row):
        return (row % 16) * PAGE + 2 * ((row % 128) // 16) + row // 128

    def read_pages():
        pages[...] = jnp.full_like(pages, -1)
        for b in range(16):
            pages[:, pl.ds(b * 16, PAGES)] = table_bt[pl.ds(b, 1)]
        hot = (lax.broadcasted_iota(jnp.int32, (192, 256), 0) == pages[...]).astype(F32)
        hot = hot.T.astype(BF16)
        gk[...] = dot_nt(hot, kc[...]).astype(BF16)
        gv[...] = dot_nt(hot, vc[...]).astype(BF16)

    def write_pages():
        hot = (lax.broadcasted_iota(jnp.int32, (192, 256), 0) == pages[...]).astype(F32)
        hot = hot.T.astype(BF16)
        kc_out[...] = dot_tn(gk[...], hot).astype(BF16)
        vc_out[...] = dot_tn(gv[...], hot).astype(BF16)

    def rope(values, cosine, sine):
        swapped = jnp.where(first_half, pltpu.roll(values, 96, 1), pltpu.roll(values, 32, 1))
        return values * cosine + swapped * sine

    def attend(unit):
        if unit % 4 == 0:
            half_loads[unit // 4].wait()
        at = (unit % 4) * 128
        values = wbuf[2 + unit // 4, at:at + 128].astype(F32)
        normed = normalize(values, again[...].astype(F32))
        q_all = dot(normed, wq[...])
        kv_all = dot_nt(normed, jnp.concatenate([wk[...], wv[...]], axis=0))
        for i in range(2):
            b = unit * 2 + i
            ctx = ctx_ref[b]
            rows = slice(i * NODES, (i + 1) * NODES)
            hot = (lax.broadcasted_iota(jnp.int32, (SPAN, NODES), 0) == depth[b:b + 1] + ctx).astype(F32).astype(BF16)
            looked = dot_tn(hot, table[...])
            both = looked[:, :256] + looked[:, 256:512] + looked[:, 512:]
            cosine, sine = both[:, :128], both[:, 128:]
            q01 = (rope(q_all[rows, :128], cosine, sine) * 0.125).astype(BF16)
            q23 = (rope(q_all[rows, 128:], cosine, sine) * 0.125).astype(BF16)
            kv_new = rope(kv_all[rows], jnp.where(low, cosine, 1.0), jnp.where(low, sine, 0.0)).astype(BF16)
            group = slice(b * 16, (b + 1) * 16)
            old_k = jnp.concatenate([gk[group, g * 128:(g + 1) * 128] for g in range(8)], axis=0).astype(F32)
            old_v = jnp.concatenate([gv[group, g * 128:(g + 1) * 128] for g in range(8)], axis=0).astype(F32)
            turned_k = pltpu.roll(old_k, HD, 1)
            turned_v = pltpu.roll(old_v, HD, 1)
            slot = slot_of(lax.broadcasted_iota(jnp.int32, (256, NODES), 0))
            place = (slot - lax.broadcasted_iota(jnp.int32, (256, NODES), 1) == ctx).astype(F32).astype(BF16)
            shifted = dot(place, kv_new)
            wide = slot_of(lax.broadcasted_iota(jnp.int32, (256, 128), 0))
            fresh = (wide >= ctx) & (wide < ctx + NODES)
            k_even = jnp.where(low, jnp.where(fresh, shifted, jnp.concatenate([old_k, turned_k], axis=0)), 0.0)
            v_odd = jnp.where(low, 0.0, jnp.where(fresh, shifted, jnp.concatenate([turned_v, old_v], axis=0)))
            k_odd = pltpu.roll(k_even, HD, 1)
            v_even = pltpu.roll(v_odd, HD, 1)
            new_k = jnp.where(low, k_even[:128], k_odd[128:]).astype(BF16)
            new_v = jnp.where(low, v_even[:128], v_odd[128:]).astype(BF16)
            for g in range(8):
                gk[group, g * 128:(g + 1) * 128] = new_k[g * 16:(g + 1) * 16]
                gv[group, g * 128:(g + 1) * 128] = new_v[g * 16:(g + 1) * 16]
            keys = (k_even.astype(BF16), k_odd.astype(BF16))
            v_even, v_odd = v_even.astype(BF16), v_odd.astype(BF16)
            tree = dot_nt(mask[b].astype(F32).astype(BF16), place)
            seen = (slot_of(lax.broadcasted_iota(jnp.int32, (NODES, 256), 1)) < ctx) | (tree > 0.5)

            def head(query, key):
                score = jnp.where(seen, dot_nt(query, key), -jnp.inf)
                weight = jnp.exp(score - jnp.max(score, axis=-1, keepdims=True))
                return weight.astype(BF16), jnp.sum(weight, axis=-1, keepdims=True)

            for pair, query in enumerate((q01, q23)):
                w_even, t_even = head(query, keys[0])
                w_odd, t_odd = head(query, keys[1])
                mixed = dot(w_even, v_even) + dot(w_odd, v_odd)
                out = (mixed / jnp.where(low, t_even, t_odd)).astype(BF16)
                att[b * NODES:(b + 1) * NODES, pair * 128:(pair + 1) * 128] = out

    def half_rows(c, which):
        return pl.ds(pl.multiple_of(c * CR + which * HALF, HALF), HALF)

    def slab(c):
        return pl.ds(c * HALF, HALF)

    def first_copy(s, c):
        return remote(psib.at[slab(c)], s1buf.at[s, slab(c)], s1_send.at[s, c], s1_recv.at[s, c], sib)

    def project(c):
        psib[slab(c)] = dot(att[half_rows(c, 1 - core)], wo[...]).astype(BF16)
        if c == 0:
            pl.semaphore_wait(barrier, 7)
        first_copy(0, c).start()
        pown[slab(c)] = dot(att[half_rows(c, core)], wo[...]).astype(BF16)

    first_cols = pl.ds(0, HD_COLS)
    last_cols = pl.ds(HD_COLS, HD_COLS)

    def stored(c, q):
        return pl.ds(pl.multiple_of(c * HALF + q * BR, BR), BR)

    def second_copy(s, c, i):
        q = (far[0], far[2], far[1], far[2], far[1], far[0])[i]
        target = peer((0, 0, 1, 1, 1, 0)[i])
        cols = (first_cols, first_cols, last_cols, last_cols, first_cols, last_cols)[i]
        return remote(pown.at[stored(c, q), cols], s2buf.at[s, c, i], s2_send.at[s, c, i], s2_recv.at[s, c, i], target)

    def pair_sum(s, c):
        first_copy(s, c).wait_recv()
        pown[slab(c)] = (pown[slab(c)].astype(F32) + s1buf[s, slab(c)].astype(F32)).astype(BF16)
        for i in (1, 3, 0, 2):
            second_copy(s, c, i).start()

    def relay(s, c):
        for i, q, cols in ((1, far[1], first_cols), (3, far[0], last_cols)):
            second_copy(s, c, i).wait_recv()
            rows = stored(c, q)
            pown[rows, cols] = (pown[rows, cols].astype(F32) + s2buf[s, c, i].astype(F32)).astype(BF16)
        for i in (4, 5):
            second_copy(s, c, i).start()

    def block_rows(c, k, q):
        return pl.ds(pl.multiple_of(c * CR + (k * 4 + q) * BR, BR), BR)

    def gather_copy(s, c, rel, rows):
        target = sib if rel == 3 else peer(rel)
        return remote(mfull.at[s, rows], mfull.at[s, rows], ag_send.at[s, c, rel], ag_recv.at[s, c, rel], target)

    def forward_copy(s, c, rel, rows):
        return remote(mfull.at[s, rows], mfull.at[s, rows], fw_send.at[s, c, rel], fw_recv.at[s, c, rel], sib)

    def finish_sum(s, c):
        for i in (0, 2, 4, 5):
            second_copy(s, c, i).wait_recv()
        rows = stored(c, chip)
        left = pown[rows, first_cols].astype(F32) + s2buf[s, c, 0].astype(F32) + s2buf[s, c, 4].astype(F32)
        right = pown[rows, last_cols].astype(F32) + s2buf[s, c, 2].astype(F32) + s2buf[s, c, 5].astype(F32)
        total = jnp.concatenate([left, right], axis=1)
        if s == 0:
            hid_loads[c].wait()
        rows = pl.ds(c * BR, BR)
        state = (hown[rows].astype(F32) + total.astype(BF16).astype(F32)).astype(BF16)
        if s == 0:
            hown[rows] = state
        gain = (mgain if s == 0 else fgain)[...].astype(F32)
        mine = block_rows(c, core, chip)
        mfull[s, mine] = normalize(state.astype(F32), gain)
        for rel in (0, 1, 3):
            gather_copy(s, c, rel, mine).start()

    def cross_copy(s, c, i, q):
        rows = block_rows(c, core, q)
        cols = (last_cols, first_cols)[i]
        part = mfull.at[s, rows, cols]
        return remote(part, part, cr_send.at[s, c, i], cr_recv.at[s, c, i], peer(1 - i))

    def forward(s, c):
        for rel in range(2):
            rows = block_rows(c, core, far[rel])
            gather_copy(s, c, rel, rows).wait_recv()
            cross_copy(s, c, rel, far[rel]).start()
            forward_copy(s, c, rel, rows).start()

    def complete(s, c):
        for i in range(2):
            cross_copy(s, c, i, far[2]).wait_recv()
        forward_copy(s, c, 2, block_rows(c, core, far[2])).start()
        gather_copy(s, c, 3, block_rows(c, 1 - core, chip)).wait_recv()
        for rel in range(3):
            forward_copy(s, c, rel, block_rows(c, 1 - core, far[rel])).wait_recv()

    def mlp(c):
        if c == 0:
            for copy in loads:
                copy.wait()

        def up(j, carry):
            cols = pl.ds(pl.multiple_of(j * 256, 256), 256)
            values = mfull[0, pl.ds(c * CR, CR)]
            gate = dot(values, wg[:, cols])
            upper = dot(values, wu[:, cols])
            pact[:, cols] = (gate * (1.0 / (1.0 + jnp.exp(-gate))) * upper).astype(BF16)
            return carry

        lax.fori_loop(0, FFN // 256, up, 0)

        def down(which, out):
            rows = pl.ds(pl.multiple_of(which * HALF, HALF), HALF)

            def one(j, carry):
                cols = pl.ds(pl.multiple_of(j * 512, 512), 512)
                out[slab(c), cols] = dot(pact[rows], wd[:, cols]).astype(BF16)
                return carry

            lax.fori_loop(0, DIM // 512, one, 0)

        first_copy(0, c).wait_send()
        for i in range(6):
            second_copy(0, c, i).wait_send()
        down(1 - core, psib)
        first_copy(1, c).start()
        down(core, pown)

    def chunk_rows(t):
        return pl.ds(pl.multiple_of((t // TILES) * PR, PR), PR)

    def multiply(logits, t):
        for part in range(2):
            piece = slice(part * TILE // 2, (part + 1) * TILE // 2)
            logits[piece, :] = dot_nt(wbuf[t % 4, piece], mfull[1, chunk_rows(t)])

    def absorb(logits, t):
        j = (t + TILES) % TILES
        rows = chunk_rows(jnp.maximum(t, 0))
        last = j == TILES - 1
        blocks = []
        for g in range(TILE // 8):
            x = logits[g * 8:(g + 1) * 8, :]
            blocks.append(jnp.where(last, -jnp.inf, x) if g * 8 < REPEAT else x)
        first = jnp.where(t < 0, 2 * VOCAB * 8, jnp.minimum(j * TILE, VOCAB - TILE))
        offset = wanted[:, rows] - first - lax.broadcasted_iota(jnp.int32, (8, PR), 0)
        before = mrun[:, rows]
        tops = [before] + [None] * 3
        for g, x in enumerate(blocks):
            old = tops[g % 4]
            tops[g % 4] = x if old is None else jnp.maximum(old, x)
        top = jnp.maximum(jnp.maximum(tops[0], tops[1]), jnp.maximum(tops[2], tops[3]))
        totals = [srun[:, rows] * jnp.exp(before - top)] + [jnp.zeros_like(top)] * 3
        picked = [prun[:, rows]] + [jnp.zeros_like(top)] * 3
        for g, x in enumerate(blocks):
            totals[g % 4] = totals[g % 4] + jnp.exp(x - top)
            hit = offset == g * 8
            if g * 8 < REPEAT:
                hit = hit & jnp.logical_not(last)
            picked[g % 4] = picked[g % 4] + jnp.where(hit, x, 0.0)
        mrun[:, rows] = top
        srun[:, rows] = (totals[0] + totals[1]) + (totals[2] + totals[3])
        prun[:, rows] = (picked[0] + picked[1]) + (picked[2] + picked[3])

    def vocab(events):
        lg1[...] = jnp.full_like(lg1, LOWEST)

        def step(i, carry):
            t = 2 * i

            @pl.when(t + 2 < PASSES * TILES)
            def _():
                tile_copy(t + 2).start()
                tile_copy(t + 3).start()

            for at, event in events:
                pl.when(i == at)(event)
            tile_copy(t).wait()
            tile_copy(t + 1).wait()
            multiply(lg0, t)
            absorb(lg1, t - 1)
            multiply(lg1, t + 1)
            absorb(lg0, t)
            return carry

        lax.fori_loop(0, PASSES * TILES // 2, step, 0)
        absorb(lg1, PASSES * TILES - 1)

    acts = {"G": read_pages, "S": write_pages, "T": attend, "O": project, "A": pair_sum, "R": relay, "B": finish_sum, "F": forward, "C": complete, "M": mlp}

    def run(plan):
        for name in plan.split():
            acts[name[0]](*(int(digit) for digit in name[1:]))

    run(BEFORE)
    vocab([(at, functools.partial(run, plan)) for at, plan in enumerate(DURING)])

    tops = mrun[...]
    top = jnp.max(tops, axis=0, keepdims=True)
    stat[0, 0:1] = top
    stat[0, 1:2] = jnp.sum(srun[...] * jnp.exp(tops - top), axis=0, keepdims=True)
    stat[0, 2:3] = jnp.sum(prun[...], axis=0, keepdims=True)

    def stat_copy(off):
        return remote(stat.at[0], stat.at[off], fin_send.at[off - 1], fin_recv.at[off - 1], (me + off) % 8)

    for off in range(1, 8):
        stat_copy(off).start()
    for off in range(1, 8):
        stat_copy(off).wait_recv()
    top = stat[0, 0:1]
    for off in range(1, 8):
        top = jnp.maximum(top, stat[off, 0:1])
    total = jnp.zeros_like(top)
    picked = jnp.zeros_like(top)
    for off in range(8):
        total = total + stat[off, 1:2] * jnp.exp(stat[off, 0:1] - top)
        picked = picked + stat[off, 2:3]
    log_norm = top + jnp.log(total)
    log_prob = picked - log_norm
    for i in range(16):
        ln_ref[pl.ds(i, 1), :] = log_norm[:, i * NODES:(i + 1) * NODES]
        lp_ref[pl.ds(i, 1), :] = log_prob[:, i * NODES:(i + 1) * NODES]

    for s in range(2):
        for c in range(CHUNKS):
            if s == 1:
                first_copy(s, c).wait_send()
            mine = block_rows(c, core, chip)
            for rel in (0, 1, 3):
                gather_copy(s, c, rel, mine).wait_send()
            for i in range(6 if s == 1 else 0):
                second_copy(s, c, i).wait_send()
            for rel in range(2):
                cross_copy(s, c, rel, far[rel]).wait_send()
            for rel in range(3):
                forward_copy(s, c, rel, block_rows(c, core, far[rel])).wait_send()
    for off in range(1, 8):
        stat_copy(off).wait_send()


def layer(*operands):
    vmem = pl.BlockSpec(memory_space=pltpu.VMEM)
    hbm = pl.BlockSpec(memory_space=pl.ANY)
    smem = pl.BlockSpec(memory_space=pltpu.SMEM)
    sem = pltpu.SemaphoreType.DMA
    return pl.pallas_call(
        layer_kernel,
        in_specs=[smem, hbm] + [vmem] * 13 + [hbm] * 3 + [vmem, hbm],
        out_specs=[vmem] * 4,
        out_shape=[jax.ShapeDtypeStruct((16, NODES), F32)] * 2 + [jax.ShapeDtypeStruct((PAGE * HD, 192), BF16)] * 2,
        scratch_shapes=[
            pltpu.VMEM((ROWS, 256), BF16),
            pltpu.VMEM((1, 256), jnp.int32),
            pltpu.VMEM((256, PAGE * HD), BF16),
            pltpu.VMEM((256, PAGE * HD), BF16),
            pltpu.VMEM((DIM, FFN), BF16),
            pltpu.VMEM((DIM, FFN), BF16),
            pltpu.VMEM((FFN, DIM), BF16),
            pltpu.VMEM((4, TILE, DIM), BF16),
            pltpu.VMEM((ROWS // 2, DIM), BF16),
            pltpu.VMEM((ROWS // 2, DIM), BF16),
            pltpu.VMEM((2, ROWS // 2, DIM), BF16),
            pltpu.VMEM((2, CHUNKS, 6, BR, HD_COLS), BF16),
            pltpu.VMEM((2, ROWS, DIM), BF16),
            pltpu.VMEM((ROWS // 8, DIM), BF16),
            pltpu.VMEM((CR, FFN), BF16),
            pltpu.VMEM((TILE, PR), F32),
            pltpu.VMEM((TILE, PR), F32),
            pltpu.VMEM((8, ROWS), F32),
            pltpu.VMEM((8, ROWS), F32),
            pltpu.VMEM((8, ROWS), F32),
            pltpu.VMEM((1, ROWS), jnp.int32),
            pltpu.VMEM((8, 8, ROWS), F32),
            sem((5 + CHUNKS,)),
            sem((4,)),
            sem((2, CHUNKS)),
            sem((2, CHUNKS)),
            sem((2, CHUNKS, 6)),
            sem((2, CHUNKS, 6)),
            sem((2, CHUNKS, 4)),
            sem((2, CHUNKS, 4)),
            sem((2, CHUNKS, 3)),
            sem((2, CHUNKS, 3)),
            sem((2, CHUNKS, 2)),
            sem((2, CHUNKS, 2)),
            sem((7,)),
            sem((7,)),
        ],
        compiler_params=pltpu.CompilerParams(collective_id=0, has_side_effects=True, vmem_limit_bytes=63 * 2**20),
        name="layer",
    )(*operands)


def solution(mesh):
    def group_step(hidden, tree_mask, depth, ctx_len, block_table, score_id, k_cache, v_cache, attn_norm, w_q, w_k, w_v, w_o, mlp_norm, w_gate, w_up, w_down, final_norm, w_lm):
        def as_stored(cache):
            return jnp.transpose(cache[:, :, 0, :], (1, 2, 0)).reshape(PAGE * HD, 192)

        def as_given(cache):
            return jnp.transpose(cache.reshape(PAGE, HD, 192), (2, 0, 1))[:, :, None, :]

        log_norm, log_prob, k_out, v_out = layer(
            ctx_len, hidden.reshape(ROWS, DIM), depth, tree_mask, block_table, score_id, as_stored(k_cache), as_stored(v_cache), attn_norm[None],
            w_q, w_k.T, w_v.T, jnp.asarray(rope_table()), w_o, mlp_norm[None], w_gate, w_up, w_down, final_norm[None], w_lm.T,
        )
        return log_norm, log_prob, as_given(k_out), as_given(v_out)

    request_spec = P("dp", None, None)
    node_spec = P("dp", None)
    cache_spec = P("dp", None, "tp", None)
    shared_spec = P(None)
    column_spec = P(None, "tp")
    row_spec = P("tp", None)
    in_specs = (request_spec, request_spec, node_spec, P("dp"), node_spec, node_spec, cache_spec, cache_spec, shared_spec, column_spec, column_spec, column_spec, row_spec, shared_spec, column_spec, column_spec, row_spec, shared_spec, column_spec)
    out_specs = (node_spec, node_spec, cache_spec, cache_spec)
    return jax.shard_map(group_step, mesh=mesh, in_specs=in_specs, out_specs=out_specs, check_vma=False)
```

```python
import functools

import jax
import jax.numpy as jnp
import numpy as np
from jax import lax
from jax.experimental import pallas as pl
from jax.experimental.pallas import tpu as pltpu
from jax.sharding import PartitionSpec as P

RMS_EPS = 1e-5
ROPE_THETA = 500000
DIM = 2048
ROWS = 1024
NODES = 64
PAGES = 12
PAGE = 16
SPAN = PAGES * PAGE
HD = 64
FFN = 1024
VOCAB = 16032
TILE = 1008
TILES = 16
REPEAT = TILES * TILE - VOCAB
LOWEST = -3e38
UP = 512
DOWN = 1024
CHUNKS = 4
PASSES = 2
PR = ROWS // PASSES
HD_COLS = DIM // 2
CR = ROWS // CHUNKS
HALF = CR // 2
BR = CR // 8
MESH = pl.DeviceIdType.MESH
F32 = jnp.float32
BF16 = jnp.bfloat16


BEFORE = "G T0 T1 O0 T2 A00 T3 O1 T4 R00 A01 T5 B00 T6 R01 T7 F00 B01 O2 O3 A02 C00 F01 R02 A03 M0 C01 A10 B02 R03 S M1 R10 A11 F02 B10 B03 R11 F10 B11 C02 F03 C10 F11 C11"
DURING = ("M2", "A12 C03 M3", "R12 A13", "B12 R13", "F12 B13", "C12 F13", "", "C13")


def rope_table():
    half = HD // 2
    freq = (np.float32(1.0) / np.power(np.float32(ROPE_THETA), np.arange(half, dtype=np.float32) * np.float32(2.0 / HD))).astype(np.float32)
    angle = (np.arange(SPAN, dtype=np.float32)[:, None] * freq[None, :]).astype(np.float32).astype(np.float64)
    cos = np.tile(np.cos(angle), (1, 4)).astype(np.float32)
    sin = np.sin(angle)
    sin = np.concatenate([-sin, sin, -sin, sin], axis=1).astype(np.float32)
    table = np.concatenate([cos, sin], axis=1)
    high = table.astype(jnp.bfloat16)
    rest = table - high.astype(np.float32)
    mid = rest.astype(jnp.bfloat16)
    low = (rest - mid.astype(np.float32)).astype(jnp.bfloat16)
    return np.concatenate([high, mid, low], axis=1)


def normalize(values, gain):
    scale = lax.rsqrt(jnp.mean(values * values, axis=-1, keepdims=True) + RMS_EPS)
    return (values * scale * gain).astype(BF16)


def dot(a, b):
    return jnp.dot(a, b, preferred_element_type=F32)


def dot_nt(a, b):
    return lax.dot_general(a, b, (((1,), (1,)), ((), ())), preferred_element_type=F32)


def dot_tn(a, b):
    return lax.dot_general(a, b, (((0,), (0,)), ((), ())), preferred_element_type=F32)


def layer_kernel(ctx_ref, hid, depth, mask, table_bt, sid, kc, vc, again, wq, wk, wv, table, wo, mgain, wg_hbm, wu_hbm, wd_hbm, fgain, wlm,
                 ln_ref, lp_ref, kc_out, vc_out,
                 att, pages, gk, gv, kmid, vmid, wg, wu, wd, wbuf, part, s1buf, s2buf, mfull, hown, pact, lg0, lg1, mrun, srun, prun, wanted, stat,
                 load_sem, tile_sem, s1_send, s1_recv, s2_send, s2_recv, ag_send, ag_recv, fw_send, fw_recv, cr_send, cr_recv, fin_send, fin_recv):
    me = lax.axis_index("tp")
    core = me % 2
    chip = me // 2
    cx = chip % 2
    cy = chip // 2
    sib = me + 1 - 2 * core
    far = (chip + 1 - 2 * cx, chip + 2 - 4 * cy, 3 - chip)

    def peer(rel):
        return 2 * far[rel] + core

    def remote(src, dst, ssem, rsem, target):
        return pltpu.make_async_remote_copy(src_ref=src, dst_ref=dst, send_sem=ssem, recv_sem=rsem, device_id={"tp": target}, device_id_type=MESH)

    barrier = pltpu.get_barrier_semaphore()
    for off in range(1, 8):
        pl.semaphore_signal(barrier, inc=1, device_id={"tp": (me + off) % 8}, device_id_type=MESH)

    loads = [
        pltpu.make_async_copy(wg_hbm, wg, load_sem.at[0]),
        pltpu.make_async_copy(wu_hbm, wu, load_sem.at[1]),
        pltpu.make_async_copy(wd_hbm, wd, load_sem.at[2]),
    ]

    def own_rows(c):
        return c * CR + (core * 4 + chip) * BR

    hid_loads = [
        pltpu.make_async_copy(hid.at[pl.ds(pl.multiple_of(own_rows(c), BR), BR)], hown.at[pl.ds(c * BR, BR)], load_sem.at[3 + c])
        for c in range(CHUNKS)
    ]
    half_loads = [
        pltpu.make_async_copy(hid.at[pl.ds(h * PR, PR)], wbuf.at[2 + h, pl.ds(0, PR)], load_sem.at[3 + CHUNKS + h])
        for h in range(2)
    ]
    for copy in half_loads + hid_loads + loads:
        copy.start()

    def tile_copy(t):
        first = jnp.minimum((t % TILES) * TILE, VOCAB - TILE)
        return pltpu.make_async_copy(wlm.at[pl.ds(pl.multiple_of(first, 16), TILE)], wbuf.at[t % 4], tile_sem.at[t % 4])

    tile_copy(0).start()
    tile_copy(1).start()

    mrun[...] = jnp.full_like(mrun, LOWEST)
    srun[...] = jnp.zeros_like(srun)
    prun[...] = jnp.zeros_like(prun)
    for i in range(16):
        wanted[:, pl.ds(i * NODES, NODES)] = sid[pl.ds(i, 1)] - me * VOCAB

    lane = lax.broadcasted_iota(jnp.int32, (1, 128), 1)
    low = lane < HD
    first_half = (lane % HD) < HD // 2

    def slot_of(row):
        return (row % 16) * PAGE + 2 * ((row % 128) // 16) + row // 128

    def read_pages():
        pages[...] = jnp.full_like(pages, -1)
        for b in range(16):
            pages[:, pl.ds(b * 16, PAGES)] = table_bt[pl.ds(b, 1)]
        hot = (lax.broadcasted_iota(jnp.int32, (192, 256), 0) == pages[...]).astype(F32)
        hot = hot.T.astype(BF16)
        gk[...] = dot_nt(hot, kc[...]).astype(BF16)
        gv[...] = dot_nt(hot, vc[...]).astype(BF16)

    cache_copies = [
        pltpu.make_async_copy(kmid, kc_out, load_sem.at[5 + CHUNKS]),
        pltpu.make_async_copy(vmid, vc_out, load_sem.at[6 + CHUNKS]),
    ]

    def write_pages():
        hot = (lax.broadcasted_iota(jnp.int32, (192, 256), 0) == pages[...]).astype(F32)
        hot = hot.T.astype(BF16)
        kmid[...] = dot_tn(gk[...], hot).astype(BF16)
        vmid[...] = dot_tn(gv[...], hot).astype(BF16)
        for copy in cache_copies:
            copy.start()

    def rope(values, cosine, sine):
        swapped = jnp.where(first_half, pltpu.roll(values, 96, 1), pltpu.roll(values, 32, 1))
        return values * cosine + swapped * sine

    def attend(unit):
        if unit % 4 == 0:
            half_loads[unit // 4].wait()
        at = (unit % 4) * 128
        values = wbuf[2 + unit // 4, at:at + 128].astype(F32)
        normed = normalize(values, again[...].astype(F32))
        q_all = dot(normed, wq[...])
        kv_all = dot_nt(normed, jnp.concatenate([wk[...], wv[...]], axis=0))
        for i in range(2):
            b = unit * 2 + i
            ctx = ctx_ref[b]
            rows = slice(i * NODES, (i + 1) * NODES)
            hot = (lax.broadcasted_iota(jnp.int32, (SPAN, NODES), 0) == depth[b:b + 1] + ctx).astype(F32).astype(BF16)
            looked = dot_tn(hot, table[...])
            both = looked[:, :256] + looked[:, 256:512] + looked[:, 512:]
            cosine, sine = both[:, :128], both[:, 128:]
            q01 = (rope(q_all[rows, :128], cosine, sine) * 0.125).astype(BF16)
            q23 = (rope(q_all[rows, 128:], cosine, sine) * 0.125).astype(BF16)
            kv_new = rope(kv_all[rows], jnp.where(low, cosine, 1.0), jnp.where(low, sine, 0.0)).astype(BF16)
            group = slice(b * 16, (b + 1) * 16)
            old_k = jnp.concatenate([gk[group, g * 128:(g + 1) * 128] for g in range(8)], axis=0).astype(F32)
            old_v = jnp.concatenate([gv[group, g * 128:(g + 1) * 128] for g in range(8)], axis=0).astype(F32)
            turned_k = pltpu.roll(old_k, HD, 1)
            turned_v = pltpu.roll(old_v, HD, 1)
            slot = slot_of(lax.broadcasted_iota(jnp.int32, (256, NODES), 0))
            place = (slot - lax.broadcasted_iota(jnp.int32, (256, NODES), 1) == ctx).astype(F32).astype(BF16)
            shifted = dot(place, kv_new)
            wide = slot_of(lax.broadcasted_iota(jnp.int32, (256, 128), 0))
            fresh = (wide >= ctx) & (wide < ctx + NODES)
            k_even = jnp.where(low, jnp.where(fresh, shifted, jnp.concatenate([old_k, turned_k], axis=0)), 0.0)
            v_odd = jnp.where(low, 0.0, jnp.where(fresh, shifted, jnp.concatenate([turned_v, old_v], axis=0)))
            k_odd = pltpu.roll(k_even, HD, 1)
            v_even = pltpu.roll(v_odd, HD, 1)
            new_k = jnp.where(low, k_even[:128], k_odd[128:]).astype(BF16)
            new_v = jnp.where(low, v_even[:128], v_odd[128:]).astype(BF16)
            for g in range(8):
                gk[group, g * 128:(g + 1) * 128] = new_k[g * 16:(g + 1) * 16]
                gv[group, g * 128:(g + 1) * 128] = new_v[g * 16:(g + 1) * 16]
            keys = (k_even.astype(BF16), k_odd.astype(BF16))
            v_even, v_odd = v_even.astype(BF16), v_odd.astype(BF16)
            tree = dot_nt(mask[b].astype(F32).astype(BF16), place)
            seen = (slot_of(lax.broadcasted_iota(jnp.int32, (NODES, 256), 1)) < ctx) | (tree > 0.5)

            def head(query, key):
                score = jnp.where(seen, dot_nt(query, key), -jnp.inf)
                weight = jnp.exp(score - jnp.max(score, axis=-1, keepdims=True))
                return weight.astype(BF16), jnp.sum(weight, axis=-1, keepdims=True)

            for pair, query in enumerate((q01, q23)):
                w_even, t_even = head(query, keys[0])
                w_odd, t_odd = head(query, keys[1])
                mixed = dot(w_even, v_even) + dot(w_odd, v_odd)
                out = (mixed / jnp.where(low, t_even, t_odd)).astype(BF16)
                att[b * NODES:(b + 1) * NODES, pair * 128:(pair + 1) * 128] = out

    def half_rows(c, which):
        return pl.ds(pl.multiple_of(c * CR + which * HALF, HALF), HALF)

    def slab(c):
        return pl.ds(c * HALF, HALF)

    def first_copy(s, c):
        return remote(part.at[half_rows(c, 1 - core)], s1buf.at[s, slab(c)], s1_send.at[s, c], s1_recv.at[s, c], sib)

    def project(c):
        rows = pl.ds(c * CR, CR)
        part[rows] = dot(att[rows], wo[...]).astype(BF16)
        if c == 0:
            pl.semaphore_wait(barrier, 7)
        first_copy(0, c).start()

    first_cols = pl.ds(0, HD_COLS)
    last_cols = pl.ds(HD_COLS, HD_COLS)

    def stored(c, q):
        return pl.ds(pl.multiple_of(c * CR + core * HALF + q * BR, BR), BR)

    def second_copy(s, c, i):
        q = (far[0], far[2], far[1], far[2], far[1], far[0])[i]
        target = peer((0, 0, 1, 1, 1, 0)[i])
        cols = (first_cols, first_cols, last_cols, last_cols, first_cols, last_cols)[i]
        return remote(part.at[stored(c, q), cols], s2buf.at[s, c, i], s2_send.at[s, c, i], s2_recv.at[s, c, i], target)

    def pair_sum(s, c):
        first_copy(s, c).wait_recv()
        rows = half_rows(c, core)
        part[rows] = (part[rows].astype(F32) + s1buf[s, slab(c)].astype(F32)).astype(BF16)
        for i in (1, 3, 0, 2):
            second_copy(s, c, i).start()

    def relay(s, c):
        for i, q, cols in ((1, far[1], first_cols), (3, far[0], last_cols)):
            second_copy(s, c, i).wait_recv()
            rows = stored(c, q)
            part[rows, cols] = (part[rows, cols].astype(F32) + s2buf[s, c, i].astype(F32)).astype(BF16)
        for i in (4, 5):
            second_copy(s, c, i).start()

    def block_rows(c, k, q):
        return pl.ds(pl.multiple_of(c * CR + (k * 4 + q) * BR, BR), BR)

    def gather_copy(s, c, rel, rows):
        target = sib if rel == 3 else peer(rel)
        return remote(mfull.at[s, rows], mfull.at[s, rows], ag_send.at[s, c, rel], ag_recv.at[s, c, rel], target)

    def forward_copy(s, c, rel, rows):
        return remote(mfull.at[s, rows], mfull.at[s, rows], fw_send.at[s, c, rel], fw_recv.at[s, c, rel], sib)

    def finish_sum(s, c):
        for i in (0, 2, 4, 5):
            second_copy(s, c, i).wait_recv()
        rows = stored(c, chip)
        left = part[rows, first_cols].astype(F32) + s2buf[s, c, 0].astype(F32) + s2buf[s, c, 4].astype(F32)
        right = part[rows, last_cols].astype(F32) + s2buf[s, c, 2].astype(F32) + s2buf[s, c, 5].astype(F32)
        total = jnp.concatenate([left, right], axis=1)
        if s == 0:
            hid_loads[c].wait()
        rows = pl.ds(c * BR, BR)
        state = (hown[rows].astype(F32) + total.astype(BF16).astype(F32)).astype(BF16)
        if s == 0:
            hown[rows] = state
        gain = (mgain if s == 0 else fgain)[...].astype(F32)
        mine = block_rows(c, core, chip)
        mfull[s, mine] = normalize(state.astype(F32), gain)
        for rel in (0, 1, 3):
            gather_copy(s, c, rel, mine).start()

    def cross_copy(s, c, i, q):
        rows = block_rows(c, core, q)
        cols = (last_cols, first_cols)[i]
        part = mfull.at[s, rows, cols]
        return remote(part, part, cr_send.at[s, c, i], cr_recv.at[s, c, i], peer(1 - i))

    def forward(s, c):
        for rel in range(2):
            rows = block_rows(c, core, far[rel])
            gather_copy(s, c, rel, rows).wait_recv()
            cross_copy(s, c, rel, far[rel]).start()
            forward_copy(s, c, rel, rows).start()

    def complete(s, c):
        for i in range(2):
            cross_copy(s, c, i, far[2]).wait_recv()
        forward_copy(s, c, 2, block_rows(c, core, far[2])).start()
        gather_copy(s, c, 3, block_rows(c, 1 - core, chip)).wait_recv()
        for rel in range(3):
            forward_copy(s, c, rel, block_rows(c, 1 - core, far[rel])).wait_recv()

    def mlp(c):
        if c == 0:
            for copy in loads:
                copy.wait()

        rows = pl.ds(c * CR, CR)

        def up(j, carry):
            cols = pl.ds(pl.multiple_of(j * UP, UP), UP)
            values = mfull[0, rows]
            gate = dot(values, wg[:, cols])
            upper = dot(values, wu[:, cols])
            pact[:, cols] = (gate * (1.0 / (1.0 + jnp.exp(-gate))) * upper).astype(BF16)
            return carry

        lax.fori_loop(0, FFN // UP, up, 0)
        first_copy(0, c).wait_send()
        for i in range(6):
            second_copy(0, c, i).wait_send()

        def down(j, carry):
            cols = pl.ds(pl.multiple_of(j * DOWN, DOWN), DOWN)
            part[rows, cols] = dot(pact[...], wd[:, cols]).astype(BF16)
            return carry

        lax.fori_loop(0, DIM // DOWN, down, 0)
        first_copy(1, c).start()

    def chunk_rows(t):
        return pl.ds(pl.multiple_of((t // TILES) * PR, PR), PR)

    def multiply(logits, t):
        for part in range(2):
            piece = slice(part * TILE // 2, (part + 1) * TILE // 2)
            logits[piece, :] = dot_nt(wbuf[t % 4, piece], mfull[1, chunk_rows(t)])

    def absorb(logits, t):
        j = (t + TILES) % TILES
        rows = chunk_rows(jnp.maximum(t, 0))
        last = j == TILES - 1
        blocks = []
        for g in range(TILE // 8):
            x = logits[g * 8:(g + 1) * 8, :]
            blocks.append(jnp.where(last, -jnp.inf, x) if g * 8 < REPEAT else x)
        first = jnp.where(t < 0, 2 * VOCAB * 8, jnp.minimum(j * TILE, VOCAB - TILE))
        offset = wanted[:, rows] - first - lax.broadcasted_iota(jnp.int32, (8, PR), 0)
        before = mrun[:, rows]
        tops = [before] + [None] * 3
        for g, x in enumerate(blocks):
            old = tops[g % 4]
            tops[g % 4] = x if old is None else jnp.maximum(old, x)
        top = jnp.maximum(jnp.maximum(tops[0], tops[1]), jnp.maximum(tops[2], tops[3]))
        totals = [srun[:, rows] * jnp.exp(before - top)] + [jnp.zeros_like(top)] * 3
        picked = [prun[:, rows]] + [jnp.zeros_like(top)] * 3
        for g, x in enumerate(blocks):
            totals[g % 4] = totals[g % 4] + jnp.exp(x - top)
            hit = offset == g * 8
            if g * 8 < REPEAT:
                hit = hit & jnp.logical_not(last)
            picked[g % 4] = picked[g % 4] + jnp.where(hit, x, 0.0)
        mrun[:, rows] = top
        srun[:, rows] = (totals[0] + totals[1]) + (totals[2] + totals[3])
        prun[:, rows] = (picked[0] + picked[1]) + (picked[2] + picked[3])

    def vocab(events):
        lg1[...] = jnp.full_like(lg1, LOWEST)

        def step(i, carry):
            t = 2 * i

            @pl.when(t + 2 < PASSES * TILES)
            def _():
                tile_copy(t + 2).start()
                tile_copy(t + 3).start()

            for at, event in events:
                pl.when(i == at)(event)
            tile_copy(t).wait()
            tile_copy(t + 1).wait()
            multiply(lg0, t)
            absorb(lg1, t - 1)
            multiply(lg1, t + 1)
            absorb(lg0, t)
            return carry

        lax.fori_loop(0, PASSES * TILES // 2, step, 0)
        absorb(lg1, PASSES * TILES - 1)

    acts = {"G": read_pages, "S": write_pages, "T": attend, "O": project, "A": pair_sum, "R": relay, "B": finish_sum, "F": forward, "C": complete, "M": mlp}

    def run(plan):
        for name in plan.split():
            acts[name[0]](*(int(digit) for digit in name[1:]))

    run(BEFORE)
    vocab([(at, functools.partial(run, plan)) for at, plan in enumerate(DURING)])

    tops = mrun[...]
    top = jnp.max(tops, axis=0, keepdims=True)
    total = jnp.sum(srun[...] * jnp.exp(tops - top), axis=0, keepdims=True)
    picked = jnp.sum(prun[...], axis=0, keepdims=True)
    for k, values in enumerate((top, total, picked)):
        for i in range(8):
            stat[0, pl.ds(8 * k + i, 1)] = values[:, i * 128:(i + 1) * 128]

    def stat_copy(off):
        return remote(stat.at[0], stat.at[off], fin_send.at[off - 1], fin_recv.at[off - 1], (me + off) % 8)

    for off in range(1, 8):
        stat_copy(off).start()
    for off in range(1, 8):
        stat_copy(off).wait_recv()
    top = stat[0, 0:8]
    for off in range(1, 8):
        top = jnp.maximum(top, stat[off, 0:8])
    total = jnp.zeros_like(top)
    picked = jnp.zeros_like(top)
    for off in range(8):
        total = total + stat[off, 8:16] * jnp.exp(stat[off, 0:8] - top)
        picked = picked + stat[off, 16:24]
    log_norm = top + jnp.log(total)
    log_prob = picked - log_norm
    for ref, values in ((ln_ref, log_norm), (lp_ref, log_prob)):
        for i in range(8):
            ref[pl.ds(2 * i, 1), :] = values[i:i + 1, 0:NODES]
            ref[pl.ds(2 * i + 1, 1), :] = values[i:i + 1, NODES:]

    for s in range(2):
        for c in range(CHUNKS):
            if s == 1:
                first_copy(s, c).wait_send()
            mine = block_rows(c, core, chip)
            for rel in (0, 1, 3):
                gather_copy(s, c, rel, mine).wait_send()
            for i in range(6 if s == 1 else 0):
                second_copy(s, c, i).wait_send()
            for rel in range(2):
                cross_copy(s, c, rel, far[rel]).wait_send()
            for rel in range(3):
                forward_copy(s, c, rel, block_rows(c, core, far[rel])).wait_send()
    for off in range(1, 8):
        stat_copy(off).wait_send()
    for copy in cache_copies:
        copy.wait()


def layer(*operands):
    vmem = pl.BlockSpec(memory_space=pltpu.VMEM)
    hbm = pl.BlockSpec(memory_space=pl.ANY)
    smem = pl.BlockSpec(memory_space=pltpu.SMEM)
    sem = pltpu.SemaphoreType.DMA
    return pl.pallas_call(
        layer_kernel,
        in_specs=[smem, hbm] + [vmem] * 13 + [hbm] * 3 + [vmem, hbm],
        out_specs=[vmem, vmem, hbm, hbm],
        out_shape=[jax.ShapeDtypeStruct((16, NODES), F32)] * 2 + [jax.ShapeDtypeStruct((PAGE * HD, 192), BF16)] * 2,
        scratch_shapes=[
            pltpu.VMEM((ROWS, 256), BF16),
            pltpu.VMEM((1, 256), jnp.int32),
            pltpu.VMEM((256, PAGE * HD), BF16),
            pltpu.VMEM((256, PAGE * HD), BF16),
            pltpu.VMEM((PAGE * HD, 192), BF16),
            pltpu.VMEM((PAGE * HD, 192), BF16),
            pltpu.VMEM((DIM, FFN), BF16),
            pltpu.VMEM((DIM, FFN), BF16),
            pltpu.VMEM((FFN, DIM), BF16),
            pltpu.VMEM((4, TILE, DIM), BF16),
            pltpu.VMEM((ROWS, DIM), BF16),
            pltpu.VMEM((2, ROWS // 2, DIM), BF16),
            pltpu.VMEM((2, CHUNKS, 6, BR, HD_COLS), BF16),
            pltpu.VMEM((2, ROWS, DIM), BF16),
            pltpu.VMEM((ROWS // 8, DIM), BF16),
            pltpu.VMEM((CR, FFN), BF16),
            pltpu.VMEM((TILE, PR), F32),
            pltpu.VMEM((TILE, PR), F32),
            pltpu.VMEM((8, ROWS), F32),
            pltpu.VMEM((8, ROWS), F32),
            pltpu.VMEM((8, ROWS), F32),
            pltpu.VMEM((1, ROWS), jnp.int32),
            pltpu.VMEM((8, 24, 128), F32),
            sem((7 + CHUNKS,)),
            sem((4,)),
            sem((2, CHUNKS)),
            sem((2, CHUNKS)),
            sem((2, CHUNKS, 6)),
            sem((2, CHUNKS, 6)),
            sem((2, CHUNKS, 4)),
            sem((2, CHUNKS, 4)),
            sem((2, CHUNKS, 3)),
            sem((2, CHUNKS, 3)),
            sem((2, CHUNKS, 2)),
            sem((2, CHUNKS, 2)),
            sem((7,)),
            sem((7,)),
        ],
        compiler_params=pltpu.CompilerParams(collective_id=0, has_side_effects=True, vmem_limit_bytes=63 * 2**20),
        name="layer",
    )(*operands)


def solution(mesh):
    def group_step(hidden, tree_mask, depth, ctx_len, block_table, score_id, k_cache, v_cache, attn_norm, w_q, w_k, w_v, w_o, mlp_norm, w_gate, w_up, w_down, final_norm, w_lm):
        def as_stored(cache):
            return jnp.transpose(cache[:, :, 0, :], (1, 2, 0)).reshape(PAGE * HD, 192)

        def as_given(cache):
            return jnp.transpose(cache.reshape(PAGE, HD, 192), (2, 0, 1))[:, :, None, :]

        log_norm, log_prob, k_out, v_out = layer(
            ctx_len, hidden.reshape(ROWS, DIM), depth, tree_mask, block_table, score_id, as_stored(k_cache), as_stored(v_cache), attn_norm[None],
            w_q, w_k.T, w_v.T, jnp.asarray(rope_table()), w_o, mlp_norm[None], w_gate, w_up, w_down, final_norm[None], w_lm.T,
        )
        return log_norm, log_prob, as_given(k_out), as_given(v_out)

    request_spec = P("dp", None, None)
    node_spec = P("dp", None)
    cache_spec = P("dp", None, "tp", None)
    shared_spec = P(None)
    column_spec = P(None, "tp")
    row_spec = P("tp", None)
    in_specs = (request_spec, request_spec, node_spec, P("dp"), node_spec, node_spec, cache_spec, cache_spec, shared_spec, column_spec, column_spec, column_spec, row_spec, shared_spec, column_spec, column_spec, row_spec, shared_spec, column_spec)
    out_specs = (node_spec, node_spec, cache_spec, cache_spec)
    return jax.shard_map(group_step, mesh=mesh, in_specs=in_specs, out_specs=out_specs, check_vma=False)
```

```python
import functools

import jax
import jax.numpy as jnp
import numpy as np
from jax import lax
from jax.experimental import pallas as pl
from jax.experimental.pallas import tpu as pltpu
from jax.sharding import PartitionSpec as P

RMS_EPS = 1e-5
ROPE_THETA = 500000
DIM = 2048
ROWS = 1024
NODES = 64
PAGES = 12
PAGE = 16
SPAN = PAGES * PAGE
HD = 64
FFN = 1024
VOCAB = 16032
TILE = 1008
TILES = 16
REPEAT = TILES * TILE - VOCAB
LOWEST = -3e38
UP = 512
DOWN = 1024
CHUNKS = 4
PASSES = 2
PR = ROWS // PASSES
HD_COLS = DIM // 2
CR = ROWS // CHUNKS
HALF = CR // 2
BR = CR // 8
MESH = pl.DeviceIdType.MESH
F32 = jnp.float32
BF16 = jnp.bfloat16


BEFORE = "G T0 T1 O0 T2 A00 T3 O1 T4 R00 A01 T5 B00 T6 R01 T7 F00 B01 O2 O3 A02 C00 F01 M0 R02 C01 A10 A03 M1 R10 A11 S B10 R11 F10 B11 R03 C10 F11 C11 B02 B03"
DURING = ("", "F02", "F03 C02 M2", "A12 C03 M3", "R12 A13", "R13 B12", "B13", "F12 F13", "C12 C13")


def rope_table():
    half = HD // 2
    freq = (np.float32(1.0) / np.power(np.float32(ROPE_THETA), np.arange(half, dtype=np.float32) * np.float32(2.0 / HD))).astype(np.float32)
    angle = (np.arange(SPAN, dtype=np.float32)[:, None] * freq[None, :]).astype(np.float32).astype(np.float64)
    cos = np.tile(np.cos(angle), (1, 4)).astype(np.float32)
    sin = np.sin(angle)
    sin = np.concatenate([-sin, sin, -sin, sin], axis=1).astype(np.float32)
    table = np.concatenate([cos, sin], axis=1)
    high = table.astype(jnp.bfloat16)
    rest = table - high.astype(np.float32)
    mid = rest.astype(jnp.bfloat16)
    low = (rest - mid.astype(np.float32)).astype(jnp.bfloat16)
    return np.concatenate([high, mid, low], axis=1)


def normalize(values, gain):
    scale = lax.rsqrt(jnp.mean(values * values, axis=-1, keepdims=True) + RMS_EPS)
    return (values * scale * gain).astype(BF16)


def dot(a, b):
    return jnp.dot(a, b, preferred_element_type=F32)


def dot_nt(a, b):
    return lax.dot_general(a, b, (((1,), (1,)), ((), ())), preferred_element_type=F32)


def dot_tn(a, b):
    return lax.dot_general(a, b, (((0,), (0,)), ((), ())), preferred_element_type=F32)


def layer_kernel(ctx_ref, hid, depth, mask, table_bt, sid, kc, vc, again, wq, wk, wv, table, wo, mgain, wg_hbm, wu_hbm, wd_hbm, fgain, wlm,
                 ln_ref, lp_ref, kc_out, vc_out,
                 att, pages, gk, gv, kmid, vmid, wg, wu, wd, wbuf, part, s1buf, s2buf, mfull, hown, pact, lg0, lg1, mrun, srun, prun, wanted, stat,
                 load_sem, tile_sem, s1_send, s1_recv, s2_send, s2_recv, ag_send, ag_recv, fw_send, fw_recv, cr_send, cr_recv, fin_send, fin_recv):
    me = lax.axis_index("tp")
    core = me % 2
    chip = me // 2
    cx = chip % 2
    cy = chip // 2
    sib = me + 1 - 2 * core
    far = (chip + 1 - 2 * cx, chip + 2 - 4 * cy, 3 - chip)

    def peer(rel):
        return 2 * far[rel] + core

    def remote(src, dst, ssem, rsem, target):
        return pltpu.make_async_remote_copy(src_ref=src, dst_ref=dst, send_sem=ssem, recv_sem=rsem, device_id={"tp": target}, device_id_type=MESH)

    barrier = pltpu.get_barrier_semaphore()
    for off in range(1, 8):
        pl.semaphore_signal(barrier, inc=1, device_id={"tp": (me + off) % 8}, device_id_type=MESH)

    loads = [
        pltpu.make_async_copy(wg_hbm, wg, load_sem.at[0]),
        pltpu.make_async_copy(wu_hbm, wu, load_sem.at[1]),
        pltpu.make_async_copy(wd_hbm, wd, load_sem.at[2]),
    ]

    def own_rows(c):
        return c * CR + (core * 4 + chip) * BR

    hid_loads = [
        pltpu.make_async_copy(hid.at[pl.ds(pl.multiple_of(own_rows(c), BR), BR)], hown.at[pl.ds(c * BR, BR)], load_sem.at[3 + c])
        for c in range(CHUNKS)
    ]
    quarter_loads = [
        pltpu.make_async_copy(hid.at[pl.ds(h * 256, 256)], wbuf.at[2 + h // 2, pl.ds(h % 2 * 256, 256)], load_sem.at[5 + CHUNKS + h])
        for h in range(4)
    ]
    for copy in quarter_loads + hid_loads + loads:
        copy.start()

    def tile_copy(t):
        first = jnp.minimum((t % TILES) * TILE, VOCAB - TILE)
        return pltpu.make_async_copy(wlm.at[pl.ds(pl.multiple_of(first, 16), TILE)], wbuf.at[t % 4], tile_sem.at[t % 4])

    tile_copy(0).start()
    tile_copy(1).start()

    mrun[...] = jnp.full_like(mrun, LOWEST)
    srun[...] = jnp.zeros_like(srun)
    prun[...] = jnp.zeros_like(prun)
    for i in range(16):
        wanted[:, pl.ds(i * NODES, NODES)] = sid[pl.ds(i, 1)] - me * VOCAB

    lane = lax.broadcasted_iota(jnp.int32, (1, 128), 1)
    low = lane < HD
    first_half = (lane % HD) < HD // 2

    def slot_of(row):
        return (row % 16) * PAGE + 2 * ((row % 128) // 16) + row // 128

    def read_pages():
        pages[...] = jnp.full_like(pages, -1)
        for b in range(16):
            pages[:, pl.ds(b * 16, PAGES)] = table_bt[pl.ds(b, 1)]
        hot = (lax.broadcasted_iota(jnp.int32, (192, 256), 0) == pages[...]).astype(F32)
        hot = hot.T.astype(BF16)
        gk[...] = dot_nt(hot, kc[...]).astype(BF16)
        gv[...] = dot_nt(hot, vc[...]).astype(BF16)

    cache_copies = [
        pltpu.make_async_copy(kmid, kc_out, load_sem.at[3 + CHUNKS]),
        pltpu.make_async_copy(vmid, vc_out, load_sem.at[4 + CHUNKS]),
    ]

    def write_pages():
        hot = (lax.broadcasted_iota(jnp.int32, (192, 256), 0) == pages[...]).astype(F32)
        hot = hot.T.astype(BF16)
        kmid[...] = dot_tn(gk[...], hot).astype(BF16)
        vmid[...] = dot_tn(gv[...], hot).astype(BF16)
        for copy in cache_copies:
            copy.start()

    def rope(values, cosine, sine):
        swapped = jnp.where(first_half, pltpu.roll(values, 96, 1), pltpu.roll(values, 32, 1))
        return values * cosine + swapped * sine

    def attend(unit):
        if unit % 2 == 0:
            quarter_loads[unit // 2].wait()
        at = (unit % 4) * 128
        values = wbuf[2 + unit // 4, at:at + 128].astype(F32)
        normed = normalize(values, again[...].astype(F32)[None])
        q_all = dot(normed, wq[...])
        kv_all = dot_nt(normed, jnp.concatenate([wk[...], wv[...]], axis=0))
        for i in range(2):
            b = unit * 2 + i
            ctx = ctx_ref[b]
            rows = slice(i * NODES, (i + 1) * NODES)
            hot = (lax.broadcasted_iota(jnp.int32, (SPAN, NODES), 0) == depth[b:b + 1] + ctx).astype(F32).astype(BF16)
            looked = dot_tn(hot, table[...])
            both = looked[:, :256] + looked[:, 256:512] + looked[:, 512:]
            cosine, sine = both[:, :128], both[:, 128:]
            q01 = (rope(q_all[rows, :128], cosine, sine) * 0.125).astype(BF16)
            q23 = (rope(q_all[rows, 128:], cosine, sine) * 0.125).astype(BF16)
            kv_new = rope(kv_all[rows], jnp.where(low, cosine, 1.0), jnp.where(low, sine, 0.0)).astype(BF16)
            group = slice(b * 16, (b + 1) * 16)
            old_k = jnp.concatenate([gk[group, g * 128:(g + 1) * 128] for g in range(8)], axis=0).astype(F32)
            old_v = jnp.concatenate([gv[group, g * 128:(g + 1) * 128] for g in range(8)], axis=0).astype(F32)
            turned_k = pltpu.roll(old_k, HD, 1)
            turned_v = pltpu.roll(old_v, HD, 1)
            slot = slot_of(lax.broadcasted_iota(jnp.int32, (256, NODES), 0))
            place = (slot - lax.broadcasted_iota(jnp.int32, (256, NODES), 1) == ctx).astype(F32).astype(BF16)
            shifted = dot(place, kv_new)
            wide = slot_of(lax.broadcasted_iota(jnp.int32, (256, 128), 0))
            fresh = (wide >= ctx) & (wide < ctx + NODES)
            k_even = jnp.where(low, jnp.where(fresh, shifted, jnp.concatenate([old_k, turned_k], axis=0)), 0.0)
            v_odd = jnp.where(low, 0.0, jnp.where(fresh, shifted, jnp.concatenate([turned_v, old_v], axis=0)))
            k_odd = pltpu.roll(k_even, HD, 1)
            v_even = pltpu.roll(v_odd, HD, 1)
            new_k = jnp.where(low, k_even[:128], k_odd[128:]).astype(BF16)
            new_v = jnp.where(low, v_even[:128], v_odd[128:]).astype(BF16)
            for g in range(8):
                gk[group, g * 128:(g + 1) * 128] = new_k[g * 16:(g + 1) * 16]
                gv[group, g * 128:(g + 1) * 128] = new_v[g * 16:(g + 1) * 16]
            keys = (k_even.astype(BF16), k_odd.astype(BF16))
            v_even, v_odd = v_even.astype(BF16), v_odd.astype(BF16)
            tree = dot_nt(mask[b].astype(F32).astype(BF16), place)
            seen = (slot_of(lax.broadcasted_iota(jnp.int32, (NODES, 256), 1)) < ctx) | (tree > 0.5)

            def head(query, key):
                score = jnp.where(seen, dot_nt(query, key), -jnp.inf)
                weight = jnp.exp(score - jnp.max(score, axis=-1, keepdims=True))
                return weight.astype(BF16), jnp.sum(weight, axis=-1, keepdims=True)

            for pair, query in enumerate((q01, q23)):
                w_even, t_even = head(query, keys[0])
                w_odd, t_odd = head(query, keys[1])
                mixed = dot(w_even, v_even) + dot(w_odd, v_odd)
                out = (mixed / jnp.where(low, t_even, t_odd)).astype(BF16)
                att[b * NODES:(b + 1) * NODES, pair * 128:(pair + 1) * 128] = out

    def half_rows(c, which):
        return pl.ds(pl.multiple_of(c * CR + which * HALF, HALF), HALF)

    def slab(c):
        return pl.ds(c * HALF, HALF)

    def first_copy(s, c):
        return remote(part.at[half_rows(c, 1 - core)], s1buf.at[s, slab(c)], s1_send.at[s, c], s1_recv.at[s, c], sib)

    def project(c):
        rows = pl.ds(c * CR, CR)
        part[rows] = dot(att[rows], wo[...]).astype(BF16)
        if c == 0:
            pl.semaphore_wait(barrier, 7)
        first_copy(0, c).start()

    first_cols = pl.ds(0, HD_COLS)
    last_cols = pl.ds(HD_COLS, HD_COLS)

    def stored(c, q):
        return pl.ds(pl.multiple_of(c * CR + core * HALF + q * BR, BR), BR)

    def second_copy(s, c, i):
        q = (far[0], far[2], far[1], far[2], far[1], far[0])[i]
        target = peer((0, 0, 1, 1, 1, 0)[i])
        cols = (first_cols, first_cols, last_cols, last_cols, first_cols, last_cols)[i]
        return remote(part.at[stored(c, q), cols], s2buf.at[s, c, i], s2_send.at[s, c, i], s2_recv.at[s, c, i], target)

    def pair_sum(s, c):
        first_copy(s, c).wait_recv()
        rows = half_rows(c, core)
        part[rows] = (part[rows].astype(F32) + s1buf[s, slab(c)].astype(F32)).astype(BF16)
        for i in (1, 3, 0, 2):
            second_copy(s, c, i).start()

    def relay(s, c):
        for i, q, cols in ((1, far[1], first_cols), (3, far[0], last_cols)):
            second_copy(s, c, i).wait_recv()
            rows = stored(c, q)
            part[rows, cols] = (part[rows, cols].astype(F32) + s2buf[s, c, i].astype(F32)).astype(BF16)
        for i in (4, 5):
            second_copy(s, c, i).start()

    def block_rows(c, k, q):
        return pl.ds(pl.multiple_of(c * CR + (k * 4 + q) * BR, BR), BR)

    def gather_copy(s, c, rel, rows):
        target = sib if rel == 3 else peer(rel)
        return remote(mfull.at[s, rows], mfull.at[s, rows], ag_send.at[s, c, rel], ag_recv.at[s, c, rel], target)

    def forward_copy(s, c, rel, rows):
        return remote(mfull.at[s, rows], mfull.at[s, rows], fw_send.at[s, c, rel], fw_recv.at[s, c, rel], sib)

    def finish_sum(s, c):
        for i in (0, 2, 4, 5):
            second_copy(s, c, i).wait_recv()
        rows = stored(c, chip)
        left = part[rows, first_cols].astype(F32) + s2buf[s, c, 0].astype(F32) + s2buf[s, c, 4].astype(F32)
        right = part[rows, last_cols].astype(F32) + s2buf[s, c, 2].astype(F32) + s2buf[s, c, 5].astype(F32)
        total = jnp.concatenate([left, right], axis=1)
        if s == 0:
            hid_loads[c].wait()
        rows = pl.ds(c * BR, BR)
        state = (hown[rows].astype(F32) + total.astype(BF16).astype(F32)).astype(BF16)
        if s == 0:
            hown[rows] = state
        gain = (mgain if s == 0 else fgain)[...].astype(F32)[None]
        mine = block_rows(c, core, chip)
        mfull[s, mine] = normalize(state.astype(F32), gain)
        for rel in (0, 1, 3):
            gather_copy(s, c, rel, mine).start()

    def cross_copy(s, c, i, q):
        rows = block_rows(c, core, q)
        cols = (last_cols, first_cols)[i]
        part = mfull.at[s, rows, cols]
        return remote(part, part, cr_send.at[s, c, i], cr_recv.at[s, c, i], peer(1 - i))

    def forward(s, c):
        for rel in range(2):
            rows = block_rows(c, core, far[rel])
            gather_copy(s, c, rel, rows).wait_recv()
            cross_copy(s, c, rel, far[rel]).start()
            forward_copy(s, c, rel, rows).start()

    def complete(s, c):
        for i in range(2):
            cross_copy(s, c, i, far[2]).wait_recv()
        forward_copy(s, c, 2, block_rows(c, core, far[2])).start()
        gather_copy(s, c, 3, block_rows(c, 1 - core, chip)).wait_recv()
        for rel in range(3):
            forward_copy(s, c, rel, block_rows(c, 1 - core, far[rel])).wait_recv()

    def mlp(c):
        if c == 0:
            for copy in loads:
                copy.wait()

        rows = pl.ds(c * CR, CR)

        def up(j, carry):
            cols = pl.ds(pl.multiple_of(j * UP, UP), UP)
            values = mfull[0, rows]
            gate = dot(values, wg[:, cols])
            upper = dot(values, wu[:, cols])
            pact[:, cols] = (gate * (1.0 / (1.0 + jnp.exp(-gate))) * upper).astype(BF16)
            return carry

        lax.fori_loop(0, FFN // UP, up, 0)
        first_copy(0, c).wait_send()
        for i in range(6):
            second_copy(0, c, i).wait_send()

        def down(j, carry):
            cols = pl.ds(pl.multiple_of(j * DOWN, DOWN), DOWN)
            part[rows, cols] = dot(pact[...], wd[:, cols]).astype(BF16)
            return carry

        lax.fori_loop(0, DIM // DOWN, down, 0)
        first_copy(1, c).start()

    def chunk_rows(t):
        return pl.ds(pl.multiple_of((t // TILES) * PR, PR), PR)

    def multiply(logits, t):
        for part in range(2):
            piece = slice(part * TILE // 2, (part + 1) * TILE // 2)
            logits[piece, :] = dot_nt(wbuf[t % 4, piece], mfull[1, chunk_rows(t)])

    def absorb(logits, t):
        j = (t + TILES) % TILES
        rows = chunk_rows(jnp.maximum(t, 0))
        last = j == TILES - 1
        blocks = []
        for g in range(TILE // 8):
            x = logits[g * 8:(g + 1) * 8, :]
            blocks.append(jnp.where(last, -jnp.inf, x) if g * 8 < REPEAT else x)
        first = jnp.where(t < 0, 2 * VOCAB * 8, jnp.minimum(j * TILE, VOCAB - TILE))
        offset = wanted[:, rows] - first - lax.broadcasted_iota(jnp.int32, (8, PR), 0)
        before = mrun[:, rows]
        tops = [before] + [None] * 3
        for g, x in enumerate(blocks):
            old = tops[g % 4]
            tops[g % 4] = x if old is None else jnp.maximum(old, x)
        top = jnp.maximum(jnp.maximum(tops[0], tops[1]), jnp.maximum(tops[2], tops[3]))
        totals = [srun[:, rows] * jnp.exp(before - top)] + [jnp.zeros_like(top)] * 3
        picked = [prun[:, rows]] + [jnp.zeros_like(top)] * 3
        for g, x in enumerate(blocks):
            totals[g % 4] = totals[g % 4] + jnp.exp(x - top)
            hit = offset == g * 8
            if g * 8 < REPEAT:
                hit = hit & jnp.logical_not(last)
            picked[g % 4] = picked[g % 4] + jnp.where(hit, x, 0.0)
        mrun[:, rows] = top
        srun[:, rows] = (totals[0] + totals[1]) + (totals[2] + totals[3])
        prun[:, rows] = (picked[0] + picked[1]) + (picked[2] + picked[3])

    def vocab(events):
        lg1[...] = jnp.full_like(lg1, LOWEST)

        def step(i, carry):
            t = 2 * i

            @pl.when(t + 2 < PASSES * TILES)
            def _():
                tile_copy(t + 2).start()
                tile_copy(t + 3).start()

            for at, event in events:
                pl.when(i == at)(event)
            tile_copy(t).wait()
            tile_copy(t + 1).wait()
            multiply(lg0, t)
            absorb(lg1, t - 1)
            multiply(lg1, t + 1)
            absorb(lg0, t)
            return carry

        lax.fori_loop(0, PASSES * TILES // 2, step, 0)
        absorb(lg1, PASSES * TILES - 1)

    acts = {"G": read_pages, "S": write_pages, "T": attend, "O": project, "A": pair_sum, "R": relay, "B": finish_sum, "F": forward, "C": complete, "M": mlp}

    def run(plan):
        for name in plan.split():
            acts[name[0]](*(int(digit) for digit in name[1:]))

    run(BEFORE)
    vocab([(at, functools.partial(run, plan)) for at, plan in enumerate(DURING)])

    tops = mrun[...]
    top = jnp.max(tops, axis=0, keepdims=True)
    total = jnp.sum(srun[...] * jnp.exp(tops - top), axis=0, keepdims=True)
    picked = jnp.sum(prun[...], axis=0, keepdims=True)
    for k, values in enumerate((top, total, picked)):
        for i in range(8):
            stat[0, pl.ds(8 * k + i, 1)] = values[:, i * 128:(i + 1) * 128]

    def stat_copy(off):
        return remote(stat.at[0], stat.at[off], fin_send.at[off - 1], fin_recv.at[off - 1], (me + off) % 8)

    for off in range(1, 8):
        stat_copy(off).start()
    for off in range(1, 8):
        stat_copy(off).wait_recv()
    top = stat[0, 0:8]
    for off in range(1, 8):
        top = jnp.maximum(top, stat[off, 0:8])
    total = jnp.zeros_like(top)
    picked = jnp.zeros_like(top)
    for off in range(8):
        total = total + stat[off, 8:16] * jnp.exp(stat[off, 0:8] - top)
        picked = picked + stat[off, 16:24]
    log_norm = top + jnp.log(total)
    log_prob = picked - log_norm
    for ref, values in ((ln_ref, log_norm), (lp_ref, log_prob)):
        for i in range(8):
            ref[pl.ds(2 * i, 1), :] = values[i:i + 1, 0:NODES]
            ref[pl.ds(2 * i + 1, 1), :] = values[i:i + 1, NODES:]

    for s in range(2):
        for c in range(CHUNKS):
            if s == 1:
                first_copy(s, c).wait_send()
            mine = block_rows(c, core, chip)
            for rel in (0, 1, 3):
                gather_copy(s, c, rel, mine).wait_send()
            for i in range(6 if s == 1 else 0):
                second_copy(s, c, i).wait_send()
            for rel in range(2):
                cross_copy(s, c, rel, far[rel]).wait_send()
            for rel in range(3):
                forward_copy(s, c, rel, block_rows(c, core, far[rel])).wait_send()
    for off in range(1, 8):
        stat_copy(off).wait_send()
    for copy in cache_copies:
        copy.wait()


def layer(*operands):
    vmem = pl.BlockSpec(memory_space=pltpu.VMEM)
    hbm = pl.BlockSpec(memory_space=pl.ANY)
    smem = pl.BlockSpec(memory_space=pltpu.SMEM)
    sem = pltpu.SemaphoreType.DMA
    return pl.pallas_call(
        layer_kernel,
        in_specs=[smem, hbm] + [vmem] * 13 + [hbm] * 3 + [vmem, hbm],
        out_specs=[vmem, vmem, hbm, hbm],
        out_shape=[jax.ShapeDtypeStruct((16, NODES), F32)] * 2 + [jax.ShapeDtypeStruct((PAGE * HD, 192), BF16)] * 2,
        scratch_shapes=[
            pltpu.VMEM((ROWS, 256), BF16),
            pltpu.VMEM((1, 256), jnp.int32),
            pltpu.VMEM((256, PAGE * HD), BF16),
            pltpu.VMEM((256, PAGE * HD), BF16),
            pltpu.VMEM((PAGE * HD, 192), BF16),
            pltpu.VMEM((PAGE * HD, 192), BF16),
            pltpu.VMEM((DIM, FFN), BF16),
            pltpu.VMEM((DIM, FFN), BF16),
            pltpu.VMEM((FFN, DIM), BF16),
            pltpu.VMEM((4, TILE, DIM), BF16),
            pltpu.VMEM((ROWS, DIM), BF16),
            pltpu.VMEM((2, ROWS // 2, DIM), BF16),
            pltpu.VMEM((2, CHUNKS, 6, BR, HD_COLS), BF16),
            pltpu.VMEM((2, ROWS, DIM), BF16),
            pltpu.VMEM((ROWS // 8, DIM), BF16),
            pltpu.VMEM((CR, FFN), BF16),
            pltpu.VMEM((TILE, PR), F32),
            pltpu.VMEM((TILE, PR), F32),
            pltpu.VMEM((8, ROWS), F32),
            pltpu.VMEM((8, ROWS), F32),
            pltpu.VMEM((8, ROWS), F32),
            pltpu.VMEM((1, ROWS), jnp.int32),
            pltpu.VMEM((8, 24, 128), F32),
            sem((9 + CHUNKS,)),
            sem((4,)),
            sem((2, CHUNKS)),
            sem((2, CHUNKS)),
            sem((2, CHUNKS, 6)),
            sem((2, CHUNKS, 6)),
            sem((2, CHUNKS, 4)),
            sem((2, CHUNKS, 4)),
            sem((2, CHUNKS, 3)),
            sem((2, CHUNKS, 3)),
            sem((2, CHUNKS, 2)),
            sem((2, CHUNKS, 2)),
            sem((7,)),
            sem((7,)),
        ],
        compiler_params=pltpu.CompilerParams(collective_id=0, has_side_effects=True, vmem_limit_bytes=63 * 2**20),
        name="layer",
    )(*operands)


def hand_over(results):
    def kernel(*refs):
        for source, target in zip(refs[:4], refs[4:]):
            target[...] = source[...]

    vmem = pl.BlockSpec(memory_space=pltpu.VMEM)
    return pl.pallas_call(
        kernel,
        in_specs=[vmem] * 4,
        out_specs=[vmem] * 4,
        out_shape=[jax.ShapeDtypeStruct(x.shape, x.dtype) for x in results],
        name="hand_over",
    )(*results)


def solution(mesh):
    def group_step(hidden, tree_mask, depth, ctx_len, block_table, score_id, k_cache, v_cache, attn_norm, w_q, w_k, w_v, w_o, mlp_norm, w_gate, w_up, w_down, final_norm, w_lm):
        def as_stored(cache):
            return jnp.transpose(cache[:, :, 0, :], (1, 2, 0)).reshape(PAGE * HD, 192)

        def as_given(cache):
            return jnp.transpose(cache.reshape(PAGE, HD, 192), (2, 0, 1))[:, :, None, :]

        log_norm, log_prob, k_out, v_out = hand_over(layer(
            ctx_len, hidden.reshape(ROWS, DIM), depth, tree_mask, block_table, score_id, as_stored(k_cache), as_stored(v_cache), attn_norm,
            w_q, w_k.T, w_v.T, jnp.asarray(rope_table()), w_o, mlp_norm, w_gate, w_up, w_down, final_norm, w_lm.T,
        ))
        return log_norm, log_prob, as_given(k_out), as_given(v_out)

    request_spec = P("dp", None, None)
    node_spec = P("dp", None)
    cache_spec = P("dp", None, "tp", None)
    shared_spec = P(None)
    column_spec = P(None, "tp")
    row_spec = P("tp", None)
    in_specs = (request_spec, request_spec, node_spec, P("dp"), node_spec, node_spec, cache_spec, cache_spec, shared_spec, column_spec, column_spec, column_spec, row_spec, shared_spec, column_spec, column_spec, row_spec, shared_spec, column_spec)
    out_specs = (node_spec, node_spec, cache_spec, cache_spec)
    return jax.shard_map(group_step, mesh=mesh, in_specs=in_specs, out_specs=out_specs, check_vma=False)
```

```python
import functools

import jax
import jax.numpy as jnp
import numpy as np
from jax import lax
from jax.experimental import pallas as pl
from jax.experimental.pallas import tpu as pltpu
from jax.sharding import PartitionSpec as P

RMS_EPS = 1e-5
ROPE_THETA = 500000
DIM = 2048
ROWS = 1024
NODES = 64
PAGES = 12
PAGE = 16
SPAN = PAGES * PAGE
HD = 64
FFN = 1024
VOCAB = 16032
TILE = 1008
TILES = 16
REPEAT = TILES * TILE - VOCAB
LOWEST = -3e38
UP = 512
DOWN = 1024
CHUNKS = 4
PASSES = 2
PR = ROWS // PASSES
HD_COLS = DIM // 2
CR = ROWS // CHUNKS
HALF = CR // 2
BR = CR // 8
MESH = pl.DeviceIdType.MESH
F32 = jnp.float32
BF16 = jnp.bfloat16


BEFORE = "G T0 T1 O0 T2 A00 T3 O1 T4 A01 T5 B00 T6 R01 T7 F00 B01 O2 O3 D00 C00 F01 A02 M0 R02 D01 A10 A03 C01 M1 R10 A11 S B10 R11 F10 B11 R03 D10 F11 D11 B02 B03 C10 C11"
DURING = ("", "F02 F03", "D02 D03 C02 M2", "A12 C03 M3", "R12 A13", "R13 B12", "B13", "F12 F13", "D12 D13 C12 C13")
DIRECT = ((0, 0),)


def rope_table():
    half = HD // 2
    freq = (np.float32(1.0) / np.power(np.float32(ROPE_THETA), np.arange(half, dtype=np.float32) * np.float32(2.0 / HD))).astype(np.float32)
    angle = (np.arange(SPAN, dtype=np.float32)[:, None] * freq[None, :]).astype(np.float32).astype(np.float64)
    cos = np.tile(np.cos(angle), (1, 4)).astype(np.float32)
    sin = np.sin(angle)
    sin = np.concatenate([-sin, sin, -sin, sin], axis=1).astype(np.float32)
    table = np.concatenate([cos, sin], axis=1)
    high = table.astype(jnp.bfloat16)
    rest = table - high.astype(np.float32)
    mid = rest.astype(jnp.bfloat16)
    low = (rest - mid.astype(np.float32)).astype(jnp.bfloat16)
    return np.concatenate([high, mid, low], axis=1)


def normalize(values, gain):
    scale = lax.rsqrt(jnp.mean(values * values, axis=-1, keepdims=True) + RMS_EPS)
    return (values * scale * gain).astype(BF16)


def dot(a, b):
    return jnp.dot(a, b, preferred_element_type=F32)


def dot_nt(a, b):
    return lax.dot_general(a, b, (((1,), (1,)), ((), ())), preferred_element_type=F32)


def dot_tn(a, b):
    return lax.dot_general(a, b, (((0,), (0,)), ((), ())), preferred_element_type=F32)


def layer_kernel(ctx_ref, hid, depth, mask, table_bt, sid, kc, vc, again, wq, wk, wv, table, wo, mgain, wg_hbm, wu_hbm, wd_hbm, fgain, wlm,
                 ln_ref, lp_ref, kc_out, vc_out,
                 att, pages, ahead, wide, across, gk, gv, kmid, vmid, wg, wu, wd, wbuf, part, s1buf, s2buf, mfull, hown, pact, lg0, lg1, mrun, srun, prun, wanted, stat,
                 load_sem, tile_sem, s1_send, s1_recv, s2_send, s2_recv, ag_send, ag_recv, fw_send, fw_recv, cr_send, cr_recv, fin_send, fin_recv):
    me = lax.axis_index("tp")
    core = me % 2
    chip = me // 2
    cx = chip % 2
    cy = chip // 2
    sib = me + 1 - 2 * core
    far = (chip + 1 - 2 * cx, chip + 2 - 4 * cy, 3 - chip)

    def peer(rel):
        return 2 * far[rel] + core

    def remote(src, dst, ssem, rsem, target):
        return pltpu.make_async_remote_copy(src_ref=src, dst_ref=dst, send_sem=ssem, recv_sem=rsem, device_id={"tp": target}, device_id_type=MESH)

    barrier = pltpu.get_barrier_semaphore()
    for off in range(1, 8):
        pl.semaphore_signal(barrier, inc=1, device_id={"tp": (me + off) % 8}, device_id_type=MESH)

    loads = [
        pltpu.make_async_copy(wg_hbm, wg, load_sem.at[0]),
        pltpu.make_async_copy(wu_hbm, wu, load_sem.at[1]),
        pltpu.make_async_copy(wd_hbm, wd, load_sem.at[2]),
    ]

    def own_rows(c):
        return c * CR + (core * 4 + chip) * BR

    hid_loads = [
        pltpu.make_async_copy(hid.at[pl.ds(pl.multiple_of(own_rows(c), BR), BR)], hown.at[pl.ds(c * BR, BR)], load_sem.at[3 + c])
        for c in range(CHUNKS)
    ]
    quarter_loads = [
        pltpu.make_async_copy(hid.at[pl.ds(h * 256, 256)], wbuf.at[2 + h // 2, pl.ds(h % 2 * 256, 256)], load_sem.at[5 + CHUNKS + h])
        for h in range(4)
    ]
    for copy in quarter_loads + hid_loads + loads:
        copy.start()

    def tile_copy(t):
        first = jnp.minimum((t % TILES) * TILE, VOCAB - TILE)
        return pltpu.make_async_copy(wlm.at[pl.ds(pl.multiple_of(first, 16), TILE)], wbuf.at[t % 4], tile_sem.at[t % 4])

    tile_copy(0).start()
    tile_copy(1).start()

    mrun[...] = jnp.full_like(mrun, LOWEST)
    srun[...] = jnp.zeros_like(srun)
    prun[...] = jnp.zeros_like(prun)
    for i in range(16):
        wanted[:, pl.ds(i * NODES, NODES)] = sid[pl.ds(i, 1)] - me * VOCAB

    lane = lax.broadcasted_iota(jnp.int32, (1, 128), 1)
    low = lane < HD
    first_half = (lane % HD) < HD // 2

    def slot_of(row):
        return (row & 15) * PAGE + ((row >> 3) & 14) + (row >> 7)

    def read_pages():
        pages[...] = jnp.full_like(pages, -1)
        ahead[...] = slot_of(lax.broadcasted_iota(jnp.int32, (256, NODES), 0)) - lax.broadcasted_iota(jnp.int32, (256, NODES), 1)
        wide[...] = slot_of(lax.broadcasted_iota(jnp.int32, (256, 128), 0))
        across[...] = slot_of(lax.broadcasted_iota(jnp.int32, (NODES, 256), 1))
        for b in range(16):
            pages[:, pl.ds(b * 16, PAGES)] = table_bt[pl.ds(b, 1)]
        hot = (lax.broadcasted_iota(jnp.int32, (192, 256), 0) == pages[...]).astype(F32)
        hot = hot.T.astype(BF16)
        gk[...] = dot_nt(hot, kc[...]).astype(BF16)
        gv[...] = dot_nt(hot, vc[...]).astype(BF16)

    cache_copies = [
        pltpu.make_async_copy(kmid, kc_out, load_sem.at[3 + CHUNKS]),
        pltpu.make_async_copy(vmid, vc_out, load_sem.at[4 + CHUNKS]),
    ]

    def write_pages():
        hot = (lax.broadcasted_iota(jnp.int32, (192, 256), 0) == pages[...]).astype(F32)
        hot = hot.T.astype(BF16)
        kmid[...] = dot_tn(gk[...], hot).astype(BF16)
        vmid[...] = dot_tn(gv[...], hot).astype(BF16)
        for copy in cache_copies:
            copy.start()

    def rope(values, cosine, sine):
        swapped = jnp.where(first_half, pltpu.roll(values, 96, 1), pltpu.roll(values, 32, 1))
        return values * cosine + swapped * sine

    def attend(unit):
        if unit % 2 == 0:
            quarter_loads[unit // 2].wait()
        at = (unit % 4) * 128
        values = wbuf[2 + unit // 4, at:at + 128].astype(F32)
        normed = normalize(values, again[...].astype(F32)[None])
        q_all = dot(normed, wq[...])
        kv_all = dot_nt(normed, jnp.concatenate([wk[...], wv[...]], axis=0))
        looks = []
        for i in range(2):
            hot = (lax.broadcasted_iota(jnp.int32, (SPAN, NODES), 0) == depth[unit * 2 + i:unit * 2 + i + 1] + ctx_ref[unit * 2 + i]).astype(F32).astype(BF16)
            looks.append(dot_tn(hot, table[...]))
        ready = []
        for i in range(2):
            b = unit * 2 + i
            ctx = ctx_ref[b]
            rows = slice(i * NODES, (i + 1) * NODES)
            looked = looks[i]
            both = looked[:, :256] + looked[:, 256:512] + looked[:, 512:]
            cosine, sine = both[:, :128], both[:, 128:]
            q01 = (rope(q_all[rows, :128], cosine, sine) * 0.125).astype(BF16)
            q23 = (rope(q_all[rows, 128:], cosine, sine) * 0.125).astype(BF16)
            kv_new = rope(kv_all[rows], jnp.where(low, cosine, 1.0), jnp.where(low, sine, 0.0)).astype(BF16)
            place = (ahead[...] == ctx).astype(F32).astype(BF16)
            shifted = dot(place, kv_new)
            tree = dot_nt(mask[b].astype(F32).astype(BF16), place)
            seen = (across[...] < ctx) | (tree > 0.5)
            ready.append((b, ctx, q01, q23, shifted, seen))
        scores, values = [], []
        for b, ctx, q01, q23, shifted, seen in ready:
            group = slice(b * 16, (b + 1) * 16)
            old_k = jnp.concatenate([gk[group, g * 128:(g + 1) * 128] for g in range(8)], axis=0).astype(F32)
            old_v = jnp.concatenate([gv[group, g * 128:(g + 1) * 128] for g in range(8)], axis=0).astype(F32)
            turned_k = pltpu.roll(old_k, HD, 1)
            turned_v = pltpu.roll(old_v, HD, 1)
            fresh = (wide[...] >= ctx) & (wide[...] < ctx + NODES)
            k_even = jnp.where(low, jnp.where(fresh, shifted, jnp.concatenate([old_k, turned_k], axis=0)), 0.0)
            v_odd = jnp.where(low, 0.0, jnp.where(fresh, shifted, jnp.concatenate([turned_v, old_v], axis=0)))
            k_odd = pltpu.roll(k_even, HD, 1)
            v_even = pltpu.roll(v_odd, HD, 1)
            keys = jnp.concatenate([k_even.astype(BF16), k_odd.astype(BF16)], axis=0)
            values.append((k_even, k_odd, v_even, v_odd))
            scores.append([dot_nt(q01, keys), dot_nt(q23, keys)])
        weights = []
        for (b, ctx, q01, q23, shifted, seen), pairs in zip(ready, scores):
            masked = [jnp.where(seen, pair[:, h * 256:(h + 1) * 256], -jnp.inf) for pair in pairs for h in range(2)]
            tops = [jnp.max(x, axis=-1, keepdims=True) for x in masked]
            weights.append([jnp.exp(x - top) for x, top in zip(masked, tops)])
        for item, parts, (k_even, k_odd, v_even, v_odd) in zip(ready, weights, values):
            b = item[0]
            both_v = jnp.concatenate([v_even.astype(BF16), v_odd.astype(BF16)], axis=0)
            sums = [jnp.sum(x, axis=-1, keepdims=True) for x in parts]
            for pair in range(2):
                joined = jnp.concatenate([parts[2 * pair].astype(BF16), parts[2 * pair + 1].astype(BF16)], axis=1)
                mixed = dot(joined, both_v)
                out = (mixed / jnp.where(low, sums[2 * pair], sums[2 * pair + 1])).astype(BF16)
                att[b * NODES:(b + 1) * NODES, pair * 128:(pair + 1) * 128] = out
        for item, (k_even, k_odd, v_even, v_odd) in zip(ready, values):
            group = slice(item[0] * 16, (item[0] + 1) * 16)
            new_k = jnp.where(low, k_even[:128], k_odd[128:]).astype(BF16)
            new_v = jnp.where(low, v_even[:128], v_odd[128:]).astype(BF16)
            for g in range(8):
                gk[group, g * 128:(g + 1) * 128] = new_k[g * 16:(g + 1) * 16]
                gv[group, g * 128:(g + 1) * 128] = new_v[g * 16:(g + 1) * 16]

    def half_rows(c, which):
        return pl.ds(pl.multiple_of(c * CR + which * HALF, HALF), HALF)

    def slab(c):
        return pl.ds(c * HALF, HALF)

    def first_copy(s, c):
        return remote(part.at[half_rows(c, 1 - core)], s1buf.at[s, slab(c)], s1_send.at[s, c], s1_recv.at[s, c], sib)

    def project(c):
        rows = pl.ds(c * CR, CR)
        part[rows] = dot(att[rows], wo[...]).astype(BF16)
        if c == 0:
            pl.semaphore_wait(barrier, 7)
        first_copy(0, c).start()

    first_cols = pl.ds(0, HD_COLS)
    last_cols = pl.ds(HD_COLS, HD_COLS)

    def stored(c, q):
        return pl.ds(pl.multiple_of(c * CR + core * HALF + q * BR, BR), BR)

    def second_copy(s, c, i):
        if (s, c) in DIRECT:
            q, target, cols = far[i // 2], peer(i // 2), (first_cols, last_cols)[i % 2]
        else:
            q = (far[0], far[2], far[1], far[2], far[1], far[0])[i]
            target = peer((0, 0, 1, 1, 1, 0)[i])
            cols = (first_cols, first_cols, last_cols, last_cols, first_cols, last_cols)[i]
        return remote(part.at[stored(c, q), cols], s2buf.at[s, c, i], s2_send.at[s, c, i], s2_recv.at[s, c, i], target)

    def pair_sum(s, c):
        first_copy(s, c).wait_recv()
        rows = half_rows(c, core)
        part[rows] = (part[rows].astype(F32) + s1buf[s, slab(c)].astype(F32)).astype(BF16)
        for i in (4, 5, 0, 1, 2, 3) if (s, c) in DIRECT else (1, 3, 0, 2):
            second_copy(s, c, i).start()

    def relay(s, c):
        for i, q, cols in ((1, far[1], first_cols), (3, far[0], last_cols)):
            second_copy(s, c, i).wait_recv()
            rows = stored(c, q)
            part[rows, cols] = (part[rows, cols].astype(F32) + s2buf[s, c, i].astype(F32)).astype(BF16)
        for i in (4, 5):
            second_copy(s, c, i).start()

    def block_rows(c, k, q):
        return pl.ds(pl.multiple_of(c * CR + (k * 4 + q) * BR, BR), BR)

    def gather_copy(s, c, rel, rows):
        target = sib if rel == 3 else peer(rel)
        return remote(mfull.at[s, rows], mfull.at[s, rows], ag_send.at[s, c, rel], ag_recv.at[s, c, rel], target)

    def forward_copy(s, c, rel, rows):
        return remote(mfull.at[s, rows], mfull.at[s, rows], fw_send.at[s, c, rel], fw_recv.at[s, c, rel], sib)

    def finish_sum(s, c):
        direct = (s, c) in DIRECT
        for i in range(6) if direct else (0, 2, 4, 5):
            second_copy(s, c, i).wait_recv()
        rows = stored(c, chip)
        left = part[rows, first_cols].astype(F32)
        for i in (0, 2, 4) if direct else (0, 4):
            left = left + s2buf[s, c, i].astype(F32)
        right = part[rows, last_cols].astype(F32)
        for i in (1, 3, 5) if direct else (2, 5):
            right = right + s2buf[s, c, i].astype(F32)
        total = jnp.concatenate([left, right], axis=1)
        if s == 0:
            hid_loads[c].wait()
        rows = pl.ds(c * BR, BR)
        state = (hown[rows].astype(F32) + total.astype(BF16).astype(F32)).astype(BF16)
        if s == 0:
            hown[rows] = state
        gain = (mgain if s == 0 else fgain)[...].astype(F32)[None]
        mine = block_rows(c, core, chip)
        mfull[s, mine] = normalize(state.astype(F32), gain)
        for rel in (0, 1, 3):
            gather_copy(s, c, rel, mine).start()

    def cross_copy(s, c, i, q):
        rows = block_rows(c, core, q)
        cols = (last_cols, first_cols)[i]
        part = mfull.at[s, rows, cols]
        return remote(part, part, cr_send.at[s, c, i], cr_recv.at[s, c, i], peer(1 - i))

    def forward(s, c):
        for rel in range(2):
            rows = block_rows(c, core, far[rel])
            gather_copy(s, c, rel, rows).wait_recv()
            cross_copy(s, c, rel, far[rel]).start()
            forward_copy(s, c, rel, rows).start()

    def forward_far(s, c):
        for i in range(2):
            cross_copy(s, c, i, far[2]).wait_recv()
        forward_copy(s, c, 2, block_rows(c, core, far[2])).start()

    def complete(s, c):
        gather_copy(s, c, 3, block_rows(c, 1 - core, chip)).wait_recv()
        for rel in range(3):
            forward_copy(s, c, rel, block_rows(c, 1 - core, far[rel])).wait_recv()

    def mlp(c):
        if c == 0:
            for copy in loads:
                copy.wait()

        rows = pl.ds(c * CR, CR)

        def up(j, carry):
            cols = pl.ds(pl.multiple_of(j * UP, UP), UP)
            values = mfull[0, rows]
            gate = dot(values, wg[:, cols])
            upper = dot(values, wu[:, cols])
            pact[:, cols] = (gate * (1.0 / (1.0 + jnp.exp(-gate))) * upper).astype(BF16)
            return carry

        lax.fori_loop(0, FFN // UP, up, 0)
        first_copy(0, c).wait_send()
        for i in range(6):
            second_copy(0, c, i).wait_send()

        def down(j, carry):
            cols = pl.ds(pl.multiple_of(j * DOWN, DOWN), DOWN)
            part[rows, cols] = dot(pact[...], wd[:, cols]).astype(BF16)
            return carry

        lax.fori_loop(0, DIM // DOWN, down, 0)
        first_copy(1, c).start()

    def chunk_rows(t):
        return pl.ds(pl.multiple_of((t // TILES) * PR, PR), PR)

    def multiply(logits, t):
        for part in range(2):
            piece = slice(part * TILE // 2, (part + 1) * TILE // 2)
            logits[piece, :] = dot_nt(wbuf[t % 4, piece], mfull[1, chunk_rows(t)])

    def absorb(logits, t):
        j = (t + TILES) % TILES
        rows = chunk_rows(jnp.maximum(t, 0))
        last = j == TILES - 1
        blocks = []
        for g in range(TILE // 8):
            x = logits[g * 8:(g + 1) * 8, :]
            blocks.append(jnp.where(last, -jnp.inf, x) if g * 8 < REPEAT else x)
        first = jnp.where(t < 0, 2 * VOCAB * 8, jnp.minimum(j * TILE, VOCAB - TILE))
        offset = wanted[:, rows] - first - lax.broadcasted_iota(jnp.int32, (8, PR), 0)
        before = mrun[:, rows]
        tops = [before] + [None] * 3
        for g, x in enumerate(blocks):
            old = tops[g % 4]
            tops[g % 4] = x if old is None else jnp.maximum(old, x)
        top = jnp.maximum(jnp.maximum(tops[0], tops[1]), jnp.maximum(tops[2], tops[3]))
        totals = [srun[:, rows] * jnp.exp(before - top)] + [jnp.zeros_like(top)] * 3
        picked = [prun[:, rows]] + [jnp.zeros_like(top)] * 3
        for g, x in enumerate(blocks):
            totals[g % 4] = totals[g % 4] + jnp.exp(x - top)
            hit = offset == g * 8
            if g * 8 < REPEAT:
                hit = hit & jnp.logical_not(last)
            picked[g % 4] = picked[g % 4] + jnp.where(hit, x, 0.0)
        mrun[:, rows] = top
        srun[:, rows] = (totals[0] + totals[1]) + (totals[2] + totals[3])
        prun[:, rows] = (picked[0] + picked[1]) + (picked[2] + picked[3])

    def vocab(events):
        lg1[...] = jnp.full_like(lg1, LOWEST)

        def step(i, carry):
            t = 2 * i

            @pl.when(t + 2 < PASSES * TILES)
            def _():
                tile_copy(t + 2).start()
                tile_copy(t + 3).start()

            for at, event in events:
                pl.when(i == at)(event)
            tile_copy(t).wait()
            tile_copy(t + 1).wait()
            multiply(lg0, t)
            absorb(lg1, t - 1)
            multiply(lg1, t + 1)
            absorb(lg0, t)
            return carry

        lax.fori_loop(0, PASSES * TILES // 2, step, 0)
        absorb(lg1, PASSES * TILES - 1)

    acts = {"G": read_pages, "S": write_pages, "T": attend, "O": project, "A": pair_sum, "R": relay, "B": finish_sum, "F": forward, "D": forward_far, "C": complete, "M": mlp}

    def run(plan):
        for name in plan.split():
            acts[name[0]](*(int(digit) for digit in name[1:]))

    run(BEFORE)
    vocab([(at, functools.partial(run, plan)) for at, plan in enumerate(DURING)])

    tops = mrun[...]
    top = jnp.max(tops, axis=0, keepdims=True)
    total = jnp.sum(srun[...] * jnp.exp(tops - top), axis=0, keepdims=True)
    picked = jnp.sum(prun[...], axis=0, keepdims=True)
    for k, values in enumerate((top, total, picked)):
        for i in range(8):
            stat[0, pl.ds(8 * k + i, 1)] = values[:, i * 128:(i + 1) * 128]

    def stat_copy(off):
        return remote(stat.at[0], stat.at[off], fin_send.at[off - 1], fin_recv.at[off - 1], (me + off) % 8)

    for off in range(1, 8):
        stat_copy(off).start()
    for off in range(1, 8):
        stat_copy(off).wait_recv()
    top = stat[0, 0:8]
    for off in range(1, 8):
        top = jnp.maximum(top, stat[off, 0:8])
    total = jnp.zeros_like(top)
    picked = jnp.zeros_like(top)
    for off in range(8):
        total = total + stat[off, 8:16] * jnp.exp(stat[off, 0:8] - top)
        picked = picked + stat[off, 16:24]
    log_norm = top + jnp.log(total)
    log_prob = picked - log_norm
    for ref, values in ((ln_ref, log_norm), (lp_ref, log_prob)):
        for i in range(8):
            ref[pl.ds(2 * i, 1), :] = values[i:i + 1, 0:NODES]
            ref[pl.ds(2 * i + 1, 1), :] = values[i:i + 1, NODES:]

    for s in range(2):
        for c in range(CHUNKS):
            if s == 1:
                first_copy(s, c).wait_send()
            mine = block_rows(c, core, chip)
            for rel in (0, 1, 3):
                gather_copy(s, c, rel, mine).wait_send()
            for i in range(6 if s == 1 else 0):
                second_copy(s, c, i).wait_send()
            for rel in range(2):
                cross_copy(s, c, rel, far[rel]).wait_send()
            for rel in range(3):
                forward_copy(s, c, rel, block_rows(c, core, far[rel])).wait_send()
    for off in range(1, 8):
        stat_copy(off).wait_send()
    for copy in cache_copies:
        copy.wait()


def layer(*operands):
    vmem = pl.BlockSpec(memory_space=pltpu.VMEM)
    hbm = pl.BlockSpec(memory_space=pl.ANY)
    smem = pl.BlockSpec(memory_space=pltpu.SMEM)
    sem = pltpu.SemaphoreType.DMA
    return pl.pallas_call(
        layer_kernel,
        in_specs=[smem, hbm] + [vmem] * 13 + [hbm] * 3 + [vmem, hbm],
        out_specs=[vmem, vmem, hbm, hbm],
        out_shape=[jax.ShapeDtypeStruct((16, NODES), F32)] * 2 + [jax.ShapeDtypeStruct((PAGE * HD, 192), BF16)] * 2,
        scratch_shapes=[
            pltpu.VMEM((ROWS, 256), BF16),
            pltpu.VMEM((1, 256), jnp.int32),
            pltpu.VMEM((256, NODES), jnp.int32),
            pltpu.VMEM((256, 128), jnp.int32),
            pltpu.VMEM((NODES, 256), jnp.int32),
            pltpu.VMEM((256, PAGE * HD), BF16),
            pltpu.VMEM((256, PAGE * HD), BF16),
            pltpu.VMEM((PAGE * HD, 192), BF16),
            pltpu.VMEM((PAGE * HD, 192), BF16),
            pltpu.VMEM((DIM, FFN), BF16),
            pltpu.VMEM((DIM, FFN), BF16),
            pltpu.VMEM((FFN, DIM), BF16),
            pltpu.VMEM((4, TILE, DIM), BF16),
            pltpu.VMEM((ROWS, DIM), BF16),
            pltpu.VMEM((2, ROWS // 2, DIM), BF16),
            pltpu.VMEM((2, CHUNKS, 6, BR, HD_COLS), BF16),
            pltpu.VMEM((2, ROWS, DIM), BF16),
            pltpu.VMEM((ROWS // 8, DIM), BF16),
            pltpu.VMEM((CR, FFN), BF16),
            pltpu.VMEM((TILE, PR), F32),
            pltpu.VMEM((TILE, PR), F32),
            pltpu.VMEM((8, ROWS), F32),
            pltpu.VMEM((8, ROWS), F32),
            pltpu.VMEM((8, ROWS), F32),
            pltpu.VMEM((1, ROWS), jnp.int32),
            pltpu.VMEM((8, 24, 128), F32),
            sem((9 + CHUNKS,)),
            sem((4,)),
            sem((2, CHUNKS)),
            sem((2, CHUNKS)),
            sem((2, CHUNKS, 6)),
            sem((2, CHUNKS, 6)),
            sem((2, CHUNKS, 4)),
            sem((2, CHUNKS, 4)),
            sem((2, CHUNKS, 3)),
            sem((2, CHUNKS, 3)),
            sem((2, CHUNKS, 2)),
            sem((2, CHUNKS, 2)),
            sem((7,)),
            sem((7,)),
        ],
        compiler_params=pltpu.CompilerParams(collective_id=0, has_side_effects=True, vmem_limit_bytes=63 * 2**20),
        name="layer",
    )(*operands)


def hand_over(results):
    def kernel(*refs):
        for source, target in zip(refs[:4], refs[4:]):
            target[...] = source[...]

    vmem = pl.BlockSpec(memory_space=pltpu.VMEM)
    return pl.pallas_call(
        kernel,
        in_specs=[vmem] * 4,
        out_specs=[vmem] * 4,
        out_shape=[jax.ShapeDtypeStruct(x.shape, x.dtype) for x in results],
        name="hand_over",
    )(*results)


def solution(mesh):
    def group_step(hidden, tree_mask, depth, ctx_len, block_table, score_id, k_cache, v_cache, attn_norm, w_q, w_k, w_v, w_o, mlp_norm, w_gate, w_up, w_down, final_norm, w_lm):
        def as_stored(cache):
            return jnp.transpose(cache[:, :, 0, :], (1, 2, 0)).reshape(PAGE * HD, 192)

        def as_given(cache):
            return jnp.transpose(cache.reshape(PAGE, HD, 192), (2, 0, 1))[:, :, None, :]

        log_norm, log_prob, k_out, v_out = hand_over(layer(
            ctx_len, hidden.reshape(ROWS, DIM), depth, tree_mask, block_table, score_id, as_stored(k_cache), as_stored(v_cache), attn_norm,
            w_q, w_k.T, w_v.T, jnp.asarray(rope_table()), w_o, mlp_norm, w_gate, w_up, w_down, final_norm, w_lm.T,
        ))
        return log_norm, log_prob, as_given(k_out), as_given(v_out)

    request_spec = P("dp", None, None)
    node_spec = P("dp", None)
    cache_spec = P("dp", None, "tp", None)
    shared_spec = P(None)
    column_spec = P(None, "tp")
    row_spec = P("tp", None)
    in_specs = (request_spec, request_spec, node_spec, P("dp"), node_spec, node_spec, cache_spec, cache_spec, shared_spec, column_spec, column_spec, column_spec, row_spec, shared_spec, column_spec, column_spec, row_spec, shared_spec, column_spec)
    out_specs = (node_spec, node_spec, cache_spec, cache_spec)
    return jax.shard_map(group_step, mesh=mesh, in_specs=in_specs, out_specs=out_specs, check_vma=False)
```
